256 devices in a mesh: row: 16 (over z, core), col: 8 (over x_lo, y), head: 2 (over x_hi).
Axes of the slice: x: 4 (x_hi: 2, x_lo: 2; x = x_hi * 2 + x_lo), y: 4, z: 8, core: 2. Of those that a mesh axis runs over, the one named last changes fastest.
Arguments:
- x_lo: float32 [24, 64, 64, 4], P('col', 'row', 'head'), may hold values from -32 to 32
- noise: float32 [24, 64, 64, 16], P('col', 'row'), may hold values from -6 to 6
- t_index: int32 [24], P('col'), may hold values from 0 to 999
- labels: int32 [24], P('col'), may hold values from 0 to 1000
- stale_kv: bfloat16 [2, 24, 32, 32, 1152], P(None, 'col', 'row', None, 'head'), may hold values from -6 to 6
- embed_w: float32 [16, 1152], replicated, may hold values from -1.5 to 1.5
- t_w1: bfloat16 [256, 1152], replicated, may hold values from -0.375 to 0.375
- t_w2: bfloat16 [1152, 1152], P(None, 'row'), may hold values from -0.1875 to 0.1875
- class_table: bfloat16 [1001, 1152], P(None, 'row'), may hold values from -6 to 6
- ada_w: bfloat16 [1152, 6912], P('row'), may hold values from -0.1875 to 0.1875
- qkv_w: bfloat16 [1152, 3, 1152], P(None, None, 'head'), may hold values from -0.1875 to 0.1875
- out_w: bfloat16 [1152, 1152], P('head'), may hold values from -0.1875 to 0.1875
- fc1_w: bfloat16 [1152, 4608], P(None, ('col', 'head')), may hold values from -0.1875 to 0.1875
- fc2_w: bfloat16 [1152, 4608], P(None, ('col', 'head')), may hold values from -0.09375 to 0.09375
Outputs:
- tokens_out: bfloat16 [24, 64, 64, 1152], P('col', 'row', 'head')
The draws below stay inside these ranges and needn't reach their ends.
All inputs are finite; a program needn't handle non-finite values.
Results may differ from the reference program's by a relative error of at most 0.025.
Values may be sent and summed in bfloat16 or wider, within the bound.
A program may use at most 128 MiB of HBM per device.

```python
import math
import jax
import jax.numpy as jnp
from jax import lax

HEADS = 16
HD = 72
D = 1152
FF = 4608
NCLASS = 1001
FREQ = 256
C = 4
TSTEPS = 1000
TR = 4
GC = 64
B = 24
GR = 64
LR = 32
LC = 32
N_ROW = 16


def draw_x_lo(key, part):
    subkeys = jax.random.split(key, 4)
    row_values = jnp.arange(GR, dtype=jnp.float32)
    row_scale = jnp.exp(math.log(3.0) * row_values / (GR - 1))
    rough = jnp.exp(jax.random.uniform(subkeys[0], (B, GR, GC, C), minval=math.log(0.5), maxval=math.log(2.0)))
    offset = jax.random.uniform(subkeys[1], (B, 1, 1, C), minval=-1.0, maxval=1.0)
    base_values = jnp.clip(jax.random.normal(subkeys[3], (B, GR, GC, C)), -4.0, 4.0)
    values = base_values * row_scale[None, :, None, None] * rough + offset
    return values.astype(jnp.float32)


def set_ends(values, own_key, least, largest):
    index_at = [jax.random.randint(jax.random.fold_in(own_key, axis), (), 0, length) for axis, length in enumerate(values.shape)]
    longest = values.shape.index(max(values.shape))
    neighbour = index_at[:longest] + [(index_at[longest] + 1) % values.shape[longest]] + index_at[longest + 1:]
    return values.at[tuple(index_at)].set(least).at[tuple(neighbour)].set(largest)


def levels(stream_key, shape, pieces, smallest, high):
    level = 1.0
    for axis_at, blocks in pieces:
        steps = jax.random.uniform(jax.random.fold_in(jax.random.fold_in(stream_key, 6), axis_at), (blocks,), jnp.float32, smallest / len(pieces), high / len(pieces))
        level = level * jnp.repeat(jnp.exp(steps), shape[axis_at] // blocks).reshape((-1,) + (1,) * (len(shape) - 1 - axis_at))
    return level


def gaussian(stream_key, shape, deviation, limit, cuts=(), kind=jnp.bfloat16):
    values = jax.random.normal(stream_key, shape, jnp.float32) * deviation
    if len(cuts) > 0:
        values = levels(stream_key, shape, cuts, -0.22, 0.18) * values
    return jnp.clip(values, min=-limit, max=limit).astype(kind)


def setup_inputs(seed: int = 0) -> dict:
    seeds = jax.random.split(jax.random.key(seed), 15)
    x_lo = draw_x_lo(jax.random.fold_in(seeds[14], 71), 0)
    noise = gaussian(seeds[1], (B, GR, GC, 4 * C), 1.0, 6.0, ((0, 8), (1, 16)), jnp.float32)
    t_index = set_ends(jax.random.randint(seeds[2], (B,), 0, TSTEPS), jax.random.fold_in(seeds[2], 1), 0, TSTEPS - 1).astype(jnp.int32)
    labels = set_ends(jax.random.randint(seeds[3], (B,), 0, NCLASS), jax.random.fold_in(seeds[3], 1), 0, NCLASS - 1).astype(jnp.int32)
    stale_kv = gaussian(seeds[4], (2, B, LR, LC, D), 1.0, 6.0, ((1, 8), (2, 16), (4, 2)))
    embed_w = gaussian(seeds[5], (4 * C, D), (4 * C) ** -0.5, 1.5, (), jnp.float32)
    t_w1 = gaussian(seeds[6], (FREQ, D), FREQ ** -0.5, 0.375)
    t_w2 = gaussian(seeds[7], (D, D), D ** -0.5, 0.1875, ((1, 16),))
    class_table = gaussian(seeds[8], (NCLASS, D), 1.0, 6.0, ((1, 16),))
    ada_w = gaussian(seeds[9], (D, 6 * D), D ** -0.5, 0.1875, ((0, 16),))
    qkv_w = gaussian(seeds[10], (D, 3, D), D ** -0.5, 0.1875, ((2, 2),))
    out_w = gaussian(seeds[11], (D, D), D ** -0.5, 0.1875, ((0, 2),))
    fc1_w = gaussian(seeds[12], (D, FF), D ** -0.5, 0.1875, ((1, 16),))
    fc2_w = gaussian(seeds[13], (D, FF), FF ** -0.5, 0.09375, ((1, 16),))
    return dict(x_lo=x_lo, noise=noise, t_index=t_index, labels=labels, stale_kv=stale_kv, embed_w=embed_w, t_w1=t_w1, t_w2=t_w2, class_table=class_table, ada_w=ada_w, qkv_w=qkv_w, out_w=out_w, fc1_w=fc1_w, fc2_w=fc2_w)


def upsample_padded(padded):
    upper = padded[:, :-2]
    middle = padded[:, 1:-1]
    lower = padded[:, 2:]
    rows_even = 0.75 * middle + 0.25 * upper
    rows_odd = 0.75 * middle + 0.25 * lower

    def widen(vertical):
        left_side = vertical[:, :, :-2]
        centre = vertical[:, :, 1:-1]
        right_side = vertical[:, :, 2:]
        return jnp.stack([0.75 * centre + 0.25 * left_side, 0.75 * centre + 0.25 * right_side], axis=3)
    stacked = jnp.stack([widen(rows_even), widen(rows_odd)], axis=3)
    return stacked.reshape(stacked.shape[0], stacked.shape[1], stacked.shape[2], 4 * stacked.shape[-1])

def noise_level(t_index):
    step_values = jnp.arange(TSTEPS, dtype=jnp.float32)
    betas = 0.0001 + (0.02 - 0.0001) * step_values / (TSTEPS - 1)
    log_keep = jnp.cumsum(jnp.log(1.0 - betas))
    picked = (jnp.arange(TSTEPS, dtype=jnp.int32)[None, :] == t_index[:, None]).astype(jnp.float32)
    return jnp.exp(lax.optimization_barrier(jnp.sum(picked * log_keep[None, :], axis=1)))

def position_table(row_pos, col_pos, width):
    quarter = width // 4
    omega = 1.0 / 10000.0 ** (jnp.arange(quarter, dtype=jnp.float32) / quarter)
    row_args = row_pos[:, None] * omega[None, :]
    col_args = col_pos[:, None] * omega[None, :]
    row_part = jnp.concatenate([jnp.sin(row_args), jnp.cos(row_args)], axis=1)
    col_part = jnp.concatenate([jnp.sin(col_args), jnp.cos(col_args)], axis=1)
    n_rows = row_pos.shape[0]
    n_cols = col_pos.shape[0]
    return jnp.concatenate([jnp.broadcast_to(row_part[:, None, :], (n_rows, n_cols, width // 2)), jnp.broadcast_to(col_part[None, :, :], (n_rows, n_cols, width // 2))], axis=2)

def condition(t_index, labels, t_w1, t_w2, class_table):
    half_freq = t_w1.shape[0] // 2
    freqs = jnp.exp(-math.log(10000.0) * jnp.arange(half_freq, dtype=jnp.float32) / half_freq)
    angles = t_index.astype(jnp.float32)[:, None] * freqs[None, :]
    freq_feat = jnp.concatenate([jnp.cos(angles), jnp.sin(angles)], axis=1).astype(jnp.bfloat16)
    t_hidden = jax.nn.silu(jnp.dot(freq_feat, t_w1, preferred_element_type=jnp.float32)).astype(jnp.bfloat16)
    t_embed = jnp.dot(t_hidden, t_w2, preferred_element_type=jnp.float32)
    onehot = (jnp.arange(class_table.shape[0], dtype=jnp.int32)[None, :] == labels[:, None]).astype(jnp.bfloat16)
    return t_embed + jnp.dot(onehot, class_table, preferred_element_type=jnp.float32)

def layer_norm(values):
    centre = lax.optimization_barrier(jnp.mean(values, axis=-1, keepdims=True))
    spread = lax.optimization_barrier(jnp.mean((values - centre) ** 2, axis=-1, keepdims=True))
    return (values - centre) * lax.rsqrt(spread + 1e-06)

def attend_image(operands):
    query, key, value, stale_key, stale_value = operands
    n_patch = N_ROW
    per_patch = TR * GC

    def to_patches(tensor):
        return tensor.reshape(n_patch, per_patch, HEADS, HD).astype(jnp.float32)
    query_p = to_patches(query)
    key_p = to_patches(key)
    value_p = to_patches(value)
    coarse_key = stale_key.reshape(LR * LC, HEADS, HD).astype(jnp.float32)
    coarse_value = stale_value.reshape(LR * LC, HEADS, HD).astype(jnp.float32)
    scale = 1.0 / math.sqrt(HD)
    fresh = jnp.einsum('pqhd,pkhd->phqk', query_p, key_p) * scale
    stale = jnp.einsum('pqhd,khd->phqk', query_p, coarse_key) * scale + math.log(4.0)
    key_patch = jnp.broadcast_to((jnp.arange(LR, dtype=jnp.int32) // (TR // 2))[:, None], (LR, LC)).reshape(LR * LC)
    own = key_patch[None, :] == jnp.arange(n_patch, dtype=jnp.int32)[:, None]
    stale = jnp.where(own[:, None, None, :], jnp.float32(-1e+30), stale)
    scores = jnp.concatenate([fresh, stale], axis=-1)
    weights = jax.nn.softmax(scores, axis=-1).astype(jnp.bfloat16).astype(jnp.float32)
    attended = jnp.einsum('phqk,pkhd->pqhd', weights[..., :per_patch], value_p)
    attended = attended + jnp.einsum('phqk,khd->pqhd', weights[..., per_patch:], coarse_value)
    return attended.reshape(GR, GC, HEADS * HD).astype(jnp.bfloat16)

def reference(x_lo, noise, t_index, labels, stale_kv, embed_w, t_w1, t_w2, class_table, ada_w, qkv_w, out_w, fc1_w, fc2_w):
    abar = noise_level(t_index)
    padded = jnp.pad(x_lo, ((0, 0), (1, 1), (1, 1), (0, 0)), mode='edge')
    upsampled = upsample_padded(padded)
    noisy = jnp.sqrt(abar)[:, None, None, None] * upsampled + jnp.sqrt(1.0 - abar)[:, None, None, None] * noise
    grouped = noisy.reshape(B, GR, GC, 4, C)
    count = 4.0 * GR * GC
    total = lax.optimization_barrier(jnp.sum(grouped, axis=(1, 2, 3)))
    squares = lax.optimization_barrier(jnp.sum(grouped * grouped, axis=(1, 2, 3)))
    centre = total / count
    spread = squares / count - centre * centre
    normed = ((grouped - centre[:, None, None, None, :]) * lax.rsqrt(spread + 1e-05)[:, None, None, None, :]).reshape(B, GR, GC, 4 * C)
    pos = position_table(jnp.arange(GR, dtype=jnp.float32), jnp.arange(GC, dtype=jnp.float32), D)
    tokens = (jnp.einsum('bijf,fd->bijd', normed, embed_w, precision=lax.Precision.HIGHEST) + pos[None]).astype(jnp.bfloat16)
    cond = condition(t_index, labels, t_w1, t_w2, class_table)
    cond_act = jax.nn.silu(cond).astype(jnp.bfloat16)
    modulation = jnp.dot(cond_act, ada_w, preferred_element_type=jnp.float32)
    shift1, scale1, gate1, shift2, scale2, gate2 = jnp.split(modulation, 6, axis=1)
    flat = tokens.astype(jnp.float32).reshape(B, GR * GC, D)
    normed1 = (layer_norm(flat) * (1.0 + scale1[:, None, :]) + shift1[:, None, :]).astype(jnp.bfloat16)
    qkv = jnp.dot(normed1.reshape(B * GR * GC, D), qkv_w.reshape(D, 3 * D), preferred_element_type=jnp.float32)
    qkv = qkv.astype(jnp.bfloat16).reshape(B, GR, GC, 3, HEADS, HD)
    stale = stale_kv.reshape(2, B, LR, LC, HEADS, HD)
    attended = lax.map(attend_image, (qkv[:, :, :, 0], qkv[:, :, :, 1], qkv[:, :, :, 2], stale[0], stale[1]))
    projected = jnp.dot(attended.reshape(B * GR * GC, D), out_w, preferred_element_type=jnp.float32).reshape(B, GR * GC, D)
    mid = (flat + gate1[:, None, :] * projected).astype(jnp.bfloat16)
    normed2 = (layer_norm(mid.astype(jnp.float32)) * (1.0 + scale2[:, None, :]) + shift2[:, None, :]).astype(jnp.bfloat16)
    hidden = jax.nn.gelu(jnp.dot(normed2.reshape(B * GR * GC, D), fc1_w, preferred_element_type=jnp.float32), approximate=True).astype(jnp.bfloat16)
    mlp_term = lax.dot_general(hidden, fc2_w, (((1,), (1,)), ((), ())), preferred_element_type=jnp.float32).reshape(B, GR * GC, D)
    tokens_out = (mid.astype(jnp.float32) + gate2[:, None, :] * mlp_term).astype(jnp.bfloat16)
    return tokens_out.reshape(B, GR, GC, D)
```

```python
import math

import jax
import jax.numpy as jnp
from jax import lax
from jax.experimental import pallas as pl
from jax.experimental.pallas import tpu as pltpu
from jax.sharding import PartitionSpec as P

HD = 72
TSTEPS = 1000


def copy_for_each(shard, axis):
    devices = lax.axis_size(axis)
    return lax.all_to_all(
        jnp.broadcast_to(shard[None], (devices, *shard.shape)), axis, 0, 0, tiled=True
    )


def laid_out(pieces, dim):
    pieces = jnp.moveaxis(pieces, 0, dim)
    shape = pieces.shape
    return pieces.reshape(*shape[:dim], shape[dim] * shape[dim + 1], *shape[dim + 2 :])


def gathered_copies(shard, axis, dim):
    pieces = copy_for_each(shard, axis)
    return laid_out(pieces, dim)


def padded_2(block, sides, width):
    for axis, dim in sides:
        count = lax.axis_size(axis)
        forward = [(i, i + 1) for i in range(count - 1)]
        backward = [(target, source) for source, target in forward]
        low = lax.ppermute(
            lax.slice_in_dim(block, block.shape[dim] - width, None, axis=dim), axis, forward
        )
        high = lax.ppermute(lax.slice_in_dim(block, 0, width, axis=dim), axis, backward)
        block = jnp.concatenate([low, block, high], axis=dim)
    return block


def taken_together(shard, axis):
    return copy_for_each(shard, axis).sum(axis=0)


def together(arrays, axis):
    line, at, done = (jnp.concatenate([a.reshape(-1) for a in arrays]), 0, [])
    total = taken_together(line, axis)
    for a in arrays:
        done.append(total[at : at + a.size].reshape(a.shape))
        at += a.size
    return tuple(done)


def gathered_total(shard, axis):
    pieces = lax.all_gather(shard, axis).astype(jnp.float32)
    return pieces.sum(axis=0)


def split_up(shard, dim, devices):
    before, after = (shard.shape[:dim], shard.shape[dim + 1 :])
    return jnp.moveaxis(shard.reshape(*before, devices, -1, *after), dim, 0)


def sent_and_summed(shard, axis, dim):
    devices = lax.axis_size(axis)
    pieces = lax.all_to_all(split_up(shard, dim, devices), axis, 0, 0, tiled=True)
    return jnp.sum(pieces.astype(jnp.float32), axis=0)


def turned_gather(arrays, axis, dims):
    turned = [jnp.moveaxis(a, dim, 0) for a, dim in zip(arrays, dims)]
    widths = [t[0].size for t in turned]
    both = jnp.concatenate([t.reshape(-1, w) for t, w in zip(turned, widths)], axis=1)
    out = lax.all_gather(both, axis, axis=0, tiled=True)
    pieces = jnp.split(out, [sum(widths[:k]) for k in range(1, len(widths))], axis=1)
    return tuple(
        (
            jnp.moveaxis(b.reshape(-1, *t.shape[1:]), 0, dim)
            for b, t, dim in zip(pieces, turned, dims)
        )
    )


def upsample_padded(padded):
    upper = padded[:, :-2]
    middle = padded[:, 1:-1]
    lower = padded[:, 2:]
    rows_even = 0.75 * middle + 0.25 * upper
    rows_odd = 0.75 * middle + 0.25 * lower

    def widen(vertical):
        left_side = vertical[:, :, :-2]
        centre = vertical[:, :, 1:-1]
        right_side = vertical[:, :, 2:]
        return jnp.stack(
            [0.75 * centre + 0.25 * left_side, 0.75 * centre + 0.25 * right_side], axis=3
        )

    stacked = jnp.stack([widen(rows_even), widen(rows_odd)], axis=3)
    return stacked.reshape(
        stacked.shape[0], stacked.shape[1], stacked.shape[2], 4 * stacked.shape[-1]
    )


def clamp_edges(padded, axis_dim, at_start, at_end):
    length = padded.shape[axis_dim]
    leading = lax.slice_in_dim(padded, 0, 1, axis=axis_dim)
    second_row = lax.slice_in_dim(padded, 1, 2, axis=axis_dim)
    trailing = lax.slice_in_dim(padded, length - 1, length, axis=axis_dim)
    before_end = lax.slice_in_dim(padded, length - 2, length - 1, axis=axis_dim)
    leading = jnp.where(at_start, second_row, leading)
    trailing = jnp.where(at_end, before_end, trailing)
    return jnp.concatenate(
        [leading, lax.slice_in_dim(padded, 1, length - 1, axis=axis_dim), trailing], axis=axis_dim
    )


def noise_level(t_index):
    step_values = jnp.arange(TSTEPS, dtype=jnp.float32)
    betas = 0.0001 + (0.02 - 0.0001) * step_values / (TSTEPS - 1)
    log_keep = jnp.cumsum(jnp.log(1.0 - betas))
    picked = (jnp.arange(TSTEPS, dtype=jnp.int32)[None, :] == t_index[:, None]).astype(jnp.float32)
    return jnp.exp(jnp.sum(picked * log_keep[None, :], axis=1))


def position_table(row_pos, col_pos, width):
    quarter = width // 4
    omega = 1.0 / 10000.0 ** (jnp.arange(quarter, dtype=jnp.float32) / quarter)
    row_args = row_pos[:, None] * omega[None, :]
    col_args = col_pos[:, None] * omega[None, :]
    row_part = jnp.concatenate([jnp.sin(row_args), jnp.cos(row_args)], axis=1)
    col_part = jnp.concatenate([jnp.sin(col_args), jnp.cos(col_args)], axis=1)
    n_rows = row_pos.shape[0]
    n_cols = col_pos.shape[0]
    return jnp.concatenate(
        [
            jnp.broadcast_to(row_part[:, None, :], (n_rows, n_cols, width // 2)),
            jnp.broadcast_to(col_part[None, :, :], (n_rows, n_cols, width // 2)),
        ],
        axis=2,
    )


def condition(t_index, labels, t_w1, t_w2, class_table):
    half_freq = t_w1.shape[0] // 2
    freqs = jnp.exp(-math.log(10000.0) * jnp.arange(half_freq, dtype=jnp.float32) / half_freq)
    angles = t_index.astype(jnp.float32)[:, None] * freqs[None, :]
    freq_feat = jnp.concatenate([jnp.cos(angles), jnp.sin(angles)], axis=1).astype(jnp.bfloat16)
    t_hidden = jax.nn.silu(jnp.dot(freq_feat, t_w1, preferred_element_type=jnp.float32)).astype(
        jnp.bfloat16
    )
    t_embed = jnp.dot(t_hidden, t_w2, preferred_element_type=jnp.float32)
    onehot = (jnp.arange(class_table.shape[0], dtype=jnp.int32)[None, :] == labels[:, None]).astype(
        jnp.bfloat16
    )
    return t_embed + jnp.dot(onehot, class_table, preferred_element_type=jnp.float32)


def layer_norm(values):
    centre = jnp.mean(values, axis=-1, keepdims=True)
    spread = jnp.mean((values - centre) ** 2, axis=-1, keepdims=True)
    return (values - centre) * lax.rsqrt(spread + 1e-06)


def spread_out(vector):
    return vector[:, None, None, :]


def fused_block(tok, mod, stale, wqkv, ow, fc1, fc2):
    D = 1152
    L2E = 1.4426950408889634
    QS = L2E / math.sqrt(HD)
    bf, f32 = jnp.bfloat16, jnp.float32
    NKEY = 256 + 15 * 64
    HID = 4608
    names = []

    def kernel(
        tok_h, mod_h, stale_h, wqkv_h, ow_h, fc1_h, fc2_h, out_ref,
        tok, mod, wq, kvb, wb, owb, qb, att, attr, n2, mid, acc, send, recv, local,
    ):
        row, col, head = lax.axis_index("row"), lax.axis_index("col"), lax.axis_index("head")
        z, core = row // 2, row % 2
        x, y = head * 2 + col // 4, col % 4

        def at(x_, y_, z_, core_):
            return (z_ * 2 + core_, (x_ % 2) * 4 + y_, x_ // 2)

        peers = {
            "sib": at(x, y, z, 1 - core),
            "zp": at(x, y, (z + 1) % 8, core),
            "zm": at(x, y, (z + 7) % 8, core),
            "ap": at((x + core) % 4, (y + 1 - core) % 4, z, core),
            "am": at((x + 4 - core) % 4, (y + 3 + core) % 4, z, core),
            "bp": at((x + 1 - core) % 4, (y + core) % 4, z, core),
            "bm": at((x + 3 + core) % 4, (y + 4 - core) % 4, z, core),
            "far": at((x + 2) % 4, y, z, core),
        }
        other = at(3 - x, y, z, core)

        copies = {}
        order = {"n": 0}

        def remote(name, src, dst, peer):
            k = order["n"]
            order["n"] = k + 1
            c = pltpu.make_async_remote_copy(
                src_ref=src, dst_ref=dst, send_sem=send.at[k], recv_sem=recv.at[k],
                device_id=peer, device_id_type=pl.DeviceIdType.MESH,
            )
            copies[name] = c
            return c

        def go(name):
            copies[name].start()

        def got(name):
            copies[name].wait_recv()

        loads = []

        def load(src, dst):
            c = pltpu.make_async_copy(src, dst, local.at[len(loads)])
            loads.append(c)
            c.start()
            return c

        half_own = pl.ds(pl.multiple_of(core * 144, 16), 144)

        def blk(group, chain, j, part=None):
            base = (group * 8 + chain * 4 + j) * 144
            lo, n = {None: (0, 144), 0: (0, 80), 1: (80, 64)}[part]
            return wb.at[:, pl.ds(base + lo, n), :]

        def ring(tag, first, sides, own, place):
            p, m = sides
            remote(tag + "1", own(None), place(1, None), p)
            remote(tag + "2", own(None), place(2, None), m)
            remote(tag + "3a", place(1, 0), place(3, 0), p)
            remote(tag + "3b", place(2, 1), place(3, 1), m)

        ap, am, bp, bm = peers["ap"], peers["am"], peers["bp"], peers["bm"]
        ring("A", 0, (ap, am), lambda part: blk(0, 0, 0, part), lambda g, part: blk(g, 0, 0, part))
        for g in range(4):
            ring(
                f"B{g}", g, (bp, bm), lambda part, g=g: blk(g, 0, 0, part),
                lambda j, part, g=g: blk(g, 0, j, part),
            )
            src = wb.at[:, pl.ds(g * 8 * 144, 576), :]
            dst = wb.at[:, pl.ds((g * 8 + 4) * 144, 576), :]
            remote(f"S{g}", src, dst, peers["sib"])

        def slot(b, s, lo=0, n=64):
            return kvb.at[b, pl.ds(256 + s * 64 + lo, n), :]

        for b in range(3):
            own = stale_h.at[b]
            zp, zm = peers["zp"], peers["zm"]
            remote(f"R1_{b}", own, slot(b, 0), zp)
            remote(f"L1_{b}", own, slot(b, 3), zm)
            for d in (1, 2):
                remote(f"R{d + 1}_{b}", slot(b, d - 1), slot(b, d), zp)
                remote(f"L{d + 1}_{b}", slot(b, 3 + d - 1), slot(b, 3 + d), zm)
            remote(f"R4_{b}", slot(b, 2, 0, 32), slot(b, 6, 0, 32), zp)
            remote(f"L4_{b}", slot(b, 5, 32, 32), slot(b, 6, 32, 32), zm)
            remote(f"C0_{b}", own, slot(b, 7), peers["sib"])
            remote(
                f"C1_{b}", kvb.at[b, pl.ds(256, 448), :], kvb.at[b, pl.ds(256 + 512, 448), :],
                peers["sib"],
            )
            remote(
                f"X{b}", att.at[b, pl.ds(pl.multiple_of((1 - head) * 128, 128), 128), :],
                attr.at[b], peers["far"],
            )
        ow_own = pl.ds(pl.multiple_of(core * 288, 16), 288)
        ow_far = pl.ds(pl.multiple_of(704 + core * 288, 16), 288)
        remote("O", ow_h.at[ow_own, :], owb.at[ow_far, :], other)
        remote("OS", owb.at[ow_far, :], owb.at[ow_far, :], peers["sib"])

        c_w1 = load(fc1_h.at[half_own, :], wb.at[0, pl.ds(0, 144), :])
        c_w2 = load(fc2_h.at[half_own, :], wb.at[1, pl.ds(0, 144), :])
        c_tok = load(tok_h, tok)
        c_mod = load(mod_h, mod)
        c_wq = load(wqkv_h, wq)
        c_ow = load(ow_h, owb.at[pl.ds(64, 576), :])
        barrier = pltpu.get_barrier_semaphore()
        for peer in peers.values():
            pl.semaphore_signal(barrier, inc=1, device_id=peer, device_id_type=pl.DeviceIdType.MESH)
        pl.semaphore_wait(barrier, len(peers))
        for b in range(3):
            go(f"R1_{b}")
            go(f"L1_{b}")
        c_w1.wait()
        c_w2.wait()
        for n in ("A1", "A2", "B01", "B02"):
            go(n)
        for b in range(3):
            go(f"C0_{b}")
        go("O")

        owb[pl.ds(0, 64), :] = jnp.zeros((64, D), bf)
        owb[pl.ds(640, 64), :] = jnp.zeros((64, D), bf)
        att[...] = jnp.zeros_like(att)
        c_tok.wait()
        c_mod.wait()
        c_wq.wait()

        def norm(v):
            centre = jnp.mean(v, axis=-1, keepdims=True)
            v = v - centre
            spread = jnp.mean(v * v, axis=-1, keepdims=True)
            return v * lax.rsqrt(spread + 1e-06)

        def modrow(b, k):
            return mod[pl.ds(b * 6 + k, 1), :]

        NT = (((1,), (1,)), ((), ()))

        def qkv(b):
            n1 = (
                norm(tok[pl.ds(b * 256, 256), :].astype(f32)) * (1.0 + modrow(b, 1)) + modrow(b, 0)
            ).astype(bf)
            q = lax.dot_general(n1, wq[pl.ds(0, 576), :], NT, preferred_element_type=f32)
            qb[b, :, pl.ds(0, 576)] = (q * QS).astype(bf)
            kv = lax.dot_general(n1, wq[pl.ds(576, 1152), :], NT, preferred_element_type=f32)
            kvb[b, pl.ds(0, 256), :] = kv.astype(bf)

        lane = lax.broadcasted_iota(jnp.int32, (1, 256), 1)

        def attend(b):
            def one(h, _):
                first = h * HD
                ks = pl.multiple_of((first // 128) * 128, 128)
                vs = pl.multiple_of(jnp.minimum(((576 + first) // 128) * 128, 896), 128)
                off = first - ks
                here = (lane >= off) & (lane < off + HD)
                q = qb[b, :, pl.ds(ks, 256)]
                q = jnp.where(here, q, jnp.zeros_like(q))
                s = lax.dot_general(
                    q, kvb[b, :, pl.ds(ks, 256)], NT, preferred_element_type=f32
                )
                fresh, old = s[:, :256], s[:, 256:]
                top = jnp.maximum(
                    jnp.max(fresh, axis=1, keepdims=True), jnp.max(old, axis=1, keepdims=True) + 2.0
                )
                p0 = jnp.exp2(fresh - top)
                p1 = jnp.exp2(old - (top - 2.0))
                mass = jnp.sum(p0, axis=1, keepdims=True) + jnp.sum(p1, axis=1, keepdims=True)
                o = jnp.dot(
                    p0.astype(bf), kvb[b, pl.ds(0, 256), pl.ds(vs, 256)],
                    preferred_element_type=f32,
                ) + jnp.dot(
                    p1.astype(bf), kvb[b, pl.ds(256, NKEY - 256), pl.ds(vs, 256)],
                    preferred_element_type=f32,
                )
                o = (o * (1.0 / mass)).astype(bf)
                voff = 576 + first - vs
                mine = (lane >= voff) & (lane < voff + HD)
                ws = pl.multiple_of(vs - 512, 128)
                att[b, :, pl.ds(ws, 256)] = jnp.where(mine, o, att[b, :, pl.ds(ws, 256)])
                return 0

            lax.fori_loop(0, 8, one, 0)

        def project(b):
            rows = pl.ds(pl.multiple_of(head * 128, 128), 128)
            p = jnp.dot(att[b, rows, :], owb[pl.ds(0, 640), :], preferred_element_type=f32)
            p = p + jnp.dot(attr[b], owb[pl.ds(640, 640), :], preferred_element_type=f32)
            t = tok[pl.ds(pl.multiple_of(b * 256 + head * 128, 128), 128), :].astype(f32)
            m = (t + modrow(b, 2) * p).astype(bf)
            mid[pl.ds(b * 128, 128), :] = m
            n = norm(m.astype(f32)) * (1.0 + modrow(b, 4)) + modrow(b, 3)
            n2[pl.ds(b * 128, 128), :] = n.astype(bf)

        def feed(first, count):
            def one(i, _):
                r = pl.ds(pl.multiple_of(first + i * 768, 256), 768)
                hid = lax.dot_general(n2[...], wb[0, r, :], NT, preferred_element_type=f32)
                hid = jax.nn.gelu(hid, approximate=True).astype(bf)
                acc[...] += jnp.dot(hid, wb[1, r, :], preferred_element_type=f32)
                return 0

            lax.fori_loop(0, count, one, 0)

        def kstep(d, b):
            got(f"R{d}_{b}")
            got(f"L{d}_{b}")
            if d < 4:
                go(f"R{d + 1}_{b}")
                go(f"L{d + 1}_{b}")

        def fwd(tag):
            got(tag + "1")
            go(tag + "3a")
            got(tag + "2")
            go(tag + "3b")

        def done(tag):
            got(tag + "3a")
            got(tag + "3b")

        qkv(0)
        kstep(1, 0)
        qkv(1)
        kstep(1, 1)
        qkv(2)
        kstep(1, 2)
        kstep(2, 0)
        fwd("A")
        for g in (1, 2):
            go(f"B{g}1")
            go(f"B{g}2")
        kstep(2, 1)
        fwd("B0")
        kstep(2, 2)
        done("A")
        go("B31")
        go("B32")
        got("O")
        go("OS")
        for b in range(3):
            kstep(3, b)
        done("B0")
        go("S0")
        for b in range(3):
            kstep(4, b)
            go(f"C1_{b}")
        fwd("B1")
        got("C0_0")
        got("C1_0")
        attend(0)
        fwd("B2")
        got("C0_1")
        got("C1_1")
        go("X0")
        attend(1)
        done("B1")
        go("S1")
        got("C0_2")
        got("C1_2")
        go("X1")
        attend(2)
        done("B2")
        go("S2")
        fwd("B3")
        c_ow.wait()
        got("OS")
        got("X0")
        project(0)
        go("X2")
        got("X1")
        project(1)
        got("X2")
        project(2)
        acc[...] = jnp.zeros_like(acc)
        got("S0")
        got("S1")
        feed(0, 3)
        done("B3")
        go("S3")
        got("S2")
        feed(2304, 1)
        got("S3")
        feed(3072, 2)
        for b in range(3):
            r = pl.ds(b * 128, 128)
            out_ref[r, :] = (mid[r, :].astype(f32) + modrow(b, 5) * acc[r, :]).astype(bf)
        for c in copies.values():
            c.wait_send()

    any_spec = pl.BlockSpec(memory_space=pl.ANY)
    n_copies = 4 + 4 * 5 + 3 * 11 + 2
    return pl.pallas_call(
        kernel,
        out_shape=jax.ShapeDtypeStruct((384, D), bf),
        in_specs=[any_spec] * 7,
        out_specs=pl.BlockSpec(memory_space=pltpu.VMEM),
        scratch_shapes=[
            pltpu.VMEM((768, D), bf),
            pltpu.VMEM((18, D), f32),
            pltpu.VMEM((1728, D), bf),
            pltpu.VMEM((3, NKEY, D), bf),
            pltpu.VMEM((2, HID, D), bf),
            pltpu.VMEM((1280, D), bf),
            pltpu.VMEM((3, 256, 640), bf),
            pltpu.VMEM((3, 256, 640), bf),
            pltpu.VMEM((3, 128, 640), bf),
            pltpu.VMEM((384, D), bf),
            pltpu.VMEM((384, D), bf),
            pltpu.VMEM((384, D), f32),
            pltpu.SemaphoreType.DMA((n_copies,)),
            pltpu.SemaphoreType.DMA((n_copies,)),
            pltpu.SemaphoreType.DMA((6,)),
        ],
        compiler_params=pltpu.CompilerParams(
            collective_id=0, has_side_effects=True, vmem_limit_bytes=64_000_000
        ),
    )(tok, mod, stale, wqkv, ow, fc1, fc2)


def body(
    x_lo,
    noise,
    t_index,
    labels,
    stale_kv,
    embed_w,
    t_w1,
    t_w2,
    class_table,
    ada_w,
    qkv_w,
    out_w,
    fc1_w,
    fc2_w,
):
    row_index = lax.axis_index("row")
    row_count = lax.axis_size("row")
    head_index = lax.axis_index("head")
    head_count = lax.axis_size("head")
    batch = noise.shape[0]
    tile_rows = noise.shape[1]
    full_cols = noise.shape[2]
    channels = x_lo.shape[3]
    width = embed_w.shape[1]
    abar = noise_level(t_index)
    gathered = gathered_copies(x_lo, "head", 2)
    padded = padded_2(gathered, (("row", 1),), 1)
    padded = clamp_edges(padded, 1, row_index == 0, row_index == row_count - 1)
    padded = jnp.pad(padded, ((0, 0), (0, 0), (1, 1), (0, 0)), mode="edge")
    upsampled = upsample_padded(padded)
    noisy = (
        jnp.sqrt(abar)[:, None, None, None] * upsampled
        + jnp.sqrt(1.0 - abar)[:, None, None, None] * noise
    )
    grouped = noisy.reshape(batch, tile_rows, full_cols, 4, channels)
    total, squares = together(
        (jnp.sum(grouped, axis=(1, 2, 3)), jnp.sum(grouped * grouped, axis=(1, 2, 3))), "row"
    )
    count = 4.0 * tile_rows * row_count * full_cols
    centre = total / count
    spread = squares / count - centre * centre
    normed = (
        (grouped - centre[:, None, None, None, :])
        * lax.rsqrt(spread + 1e-05)[:, None, None, None, :]
    ).reshape(batch, tile_rows, full_cols, 4 * channels)
    row_pos = (row_index * tile_rows + jnp.arange(tile_rows, dtype=jnp.int32)).astype(jnp.float32)
    col_pos = jnp.arange(full_cols, dtype=jnp.float32)
    pos = position_table(row_pos, col_pos, width)
    tokens = (jnp.einsum("bijf,fd->bijd", normed, embed_w) + pos[None]).astype(jnp.bfloat16)
    cond_part = condition(t_index, labels, t_w1, t_w2, class_table)
    cond_act = jax.nn.silu(cond_part).astype(jnp.bfloat16)
    part = jnp.dot(cond_act, ada_w, preferred_element_type=jnp.float32)
    part = part.reshape(batch, row_count, -1).transpose(1, 0, 2)
    piece = lax.all_to_all(part, "row", 0, 0, tiled=True).sum(axis=0)
    modulation = copy_for_each(piece, "row").transpose(1, 0, 2).reshape(batch * 6, width)
    half = full_cols // head_count
    tok = tokens.reshape(batch, tile_rows, head_count, half, width).transpose(0, 2, 1, 3, 4)
    tok = tok.reshape(batch * tile_rows * full_cols, width)
    local_width = qkv_w.shape[2]
    stale = stale_kv.transpose(1, 2, 3, 0, 4).reshape(batch, -1, 2 * local_width)
    out = fused_block(
        tok,
        modulation,
        stale,
        qkv_w.transpose(1, 2, 0).reshape(3 * local_width, width),
        out_w,
        fc1_w.T,
        fc2_w.T,
    )
    return out.reshape(batch, tile_rows, half, width)


def solution(mesh):
    placed = (
        P("col", "row", "head", None),
        P("col", "row", None, None),
        P("col"),
        P("col"),
        P(None, "col", "row", None, "head"),
        P(),
        P(),
        P(None, "row"),
        P(None, "row"),
        P("row", None),
        P(None, None, "head"),
        P("head", None),
        P(None, ("col", "head")),
        P(None, ("col", "head")),
    )
    return jax.shard_map(
        body, mesh=mesh, in_specs=placed, out_specs=P("col", "row", "head", None), check_vma=False
    )
```

```python
import math

import jax
import jax.numpy as jnp
from jax import lax
from jax.experimental import pallas as pl
from jax.experimental.pallas import tpu as pltpu
from jax.sharding import PartitionSpec as P

HD = 72
TSTEPS = 1000


def copy_for_each(shard, axis):
    devices = lax.axis_size(axis)
    return lax.all_to_all(
        jnp.broadcast_to(shard[None], (devices, *shard.shape)), axis, 0, 0, tiled=True
    )


def laid_out(pieces, dim):
    pieces = jnp.moveaxis(pieces, 0, dim)
    shape = pieces.shape
    return pieces.reshape(*shape[:dim], shape[dim] * shape[dim + 1], *shape[dim + 2 :])


def gathered_copies(shard, axis, dim):
    pieces = copy_for_each(shard, axis)
    return laid_out(pieces, dim)


def padded_2(block, sides, width):
    for axis, dim in sides:
        count = lax.axis_size(axis)
        forward = [(i, i + 1) for i in range(count - 1)]
        backward = [(target, source) for source, target in forward]
        low = lax.ppermute(
            lax.slice_in_dim(block, block.shape[dim] - width, None, axis=dim), axis, forward
        )
        high = lax.ppermute(lax.slice_in_dim(block, 0, width, axis=dim), axis, backward)
        block = jnp.concatenate([low, block, high], axis=dim)
    return block


def taken_together(shard, axis):
    return copy_for_each(shard, axis).sum(axis=0)


def together(arrays, axis):
    line, at, done = (jnp.concatenate([a.reshape(-1) for a in arrays]), 0, [])
    total = taken_together(line, axis)
    for a in arrays:
        done.append(total[at : at + a.size].reshape(a.shape))
        at += a.size
    return tuple(done)


def gathered_total(shard, axis):
    pieces = lax.all_gather(shard, axis).astype(jnp.float32)
    return pieces.sum(axis=0)


def split_up(shard, dim, devices):
    before, after = (shard.shape[:dim], shard.shape[dim + 1 :])
    return jnp.moveaxis(shard.reshape(*before, devices, -1, *after), dim, 0)


def sent_and_summed(shard, axis, dim):
    devices = lax.axis_size(axis)
    pieces = lax.all_to_all(split_up(shard, dim, devices), axis, 0, 0, tiled=True)
    return jnp.sum(pieces.astype(jnp.float32), axis=0)


def turned_gather(arrays, axis, dims):
    turned = [jnp.moveaxis(a, dim, 0) for a, dim in zip(arrays, dims)]
    widths = [t[0].size for t in turned]
    both = jnp.concatenate([t.reshape(-1, w) for t, w in zip(turned, widths)], axis=1)
    out = lax.all_gather(both, axis, axis=0, tiled=True)
    pieces = jnp.split(out, [sum(widths[:k]) for k in range(1, len(widths))], axis=1)
    return tuple(
        (
            jnp.moveaxis(b.reshape(-1, *t.shape[1:]), 0, dim)
            for b, t, dim in zip(pieces, turned, dims)
        )
    )


def upsample_padded(padded):
    upper = padded[:, :-2]
    middle = padded[:, 1:-1]
    lower = padded[:, 2:]
    rows_even = 0.75 * middle + 0.25 * upper
    rows_odd = 0.75 * middle + 0.25 * lower

    def widen(vertical):
        left_side = vertical[:, :, :-2]
        centre = vertical[:, :, 1:-1]
        right_side = vertical[:, :, 2:]
        return jnp.stack(
            [0.75 * centre + 0.25 * left_side, 0.75 * centre + 0.25 * right_side], axis=3
        )

    stacked = jnp.stack([widen(rows_even), widen(rows_odd)], axis=3)
    return stacked.reshape(
        stacked.shape[0], stacked.shape[1], stacked.shape[2], 4 * stacked.shape[-1]
    )


def clamp_edges(padded, axis_dim, at_start, at_end):
    length = padded.shape[axis_dim]
    leading = lax.slice_in_dim(padded, 0, 1, axis=axis_dim)
    second_row = lax.slice_in_dim(padded, 1, 2, axis=axis_dim)
    trailing = lax.slice_in_dim(padded, length - 1, length, axis=axis_dim)
    before_end = lax.slice_in_dim(padded, length - 2, length - 1, axis=axis_dim)
    leading = jnp.where(at_start, second_row, leading)
    trailing = jnp.where(at_end, before_end, trailing)
    return jnp.concatenate(
        [leading, lax.slice_in_dim(padded, 1, length - 1, axis=axis_dim), trailing], axis=axis_dim
    )


def noise_level(t_index):
    step_values = jnp.arange(TSTEPS, dtype=jnp.float32)
    betas = 0.0001 + (0.02 - 0.0001) * step_values / (TSTEPS - 1)
    log_keep = jnp.cumsum(jnp.log(1.0 - betas))
    picked = (jnp.arange(TSTEPS, dtype=jnp.int32)[None, :] == t_index[:, None]).astype(jnp.float32)
    return jnp.exp(jnp.sum(picked * log_keep[None, :], axis=1))


def position_table(row_pos, col_pos, width):
    quarter = width // 4
    omega = 1.0 / 10000.0 ** (jnp.arange(quarter, dtype=jnp.float32) / quarter)
    row_args = row_pos[:, None] * omega[None, :]
    col_args = col_pos[:, None] * omega[None, :]
    row_part = jnp.concatenate([jnp.sin(row_args), jnp.cos(row_args)], axis=1)
    col_part = jnp.concatenate([jnp.sin(col_args), jnp.cos(col_args)], axis=1)
    n_rows = row_pos.shape[0]
    n_cols = col_pos.shape[0]
    return jnp.concatenate(
        [
            jnp.broadcast_to(row_part[:, None, :], (n_rows, n_cols, width // 2)),
            jnp.broadcast_to(col_part[None, :, :], (n_rows, n_cols, width // 2)),
        ],
        axis=2,
    )


def condition(t_index, labels, t_w1, t_w2, class_table):
    half_freq = t_w1.shape[0] // 2
    freqs = jnp.exp(-math.log(10000.0) * jnp.arange(half_freq, dtype=jnp.float32) / half_freq)
    angles = t_index.astype(jnp.float32)[:, None] * freqs[None, :]
    freq_feat = jnp.concatenate([jnp.cos(angles), jnp.sin(angles)], axis=1).astype(jnp.bfloat16)
    t_hidden = jax.nn.silu(jnp.dot(freq_feat, t_w1, preferred_element_type=jnp.float32)).astype(
        jnp.bfloat16
    )
    t_embed = jnp.dot(t_hidden, t_w2, preferred_element_type=jnp.float32)
    onehot = (jnp.arange(class_table.shape[0], dtype=jnp.int32)[None, :] == labels[:, None]).astype(
        jnp.bfloat16
    )
    return t_embed + jnp.dot(onehot, class_table, preferred_element_type=jnp.float32)


def layer_norm(values):
    centre = jnp.mean(values, axis=-1, keepdims=True)
    spread = jnp.mean((values - centre) ** 2, axis=-1, keepdims=True)
    return (values - centre) * lax.rsqrt(spread + 1e-06)


def spread_out(vector):
    return vector[:, None, None, :]


def fused_block(levels, x_lo, noise, embed, pos, part, stale, wqkv, ow, fc1, fc2):
    D = 1152
    L2E = 1.4426950408889634
    QS = L2E / math.sqrt(HD)
    bf, f32 = jnp.bfloat16, jnp.float32
    NKEY = 256 + 15 * 64
    HID = 4608
    UNROLL = 2

    def kernel(
        levels_s, x_h, noise_h, embed_h, pos_h, part_h, stale_h, wqkv_h, ow_h, fc1_h, fc2_h, out_ref,
        xn, nz, emb, pos, part, rsb, redc, modp, st, stb, noisy,
        tok, wq, kvb, wb, owb, qb, att, attr, n2, mid, acc, send, recv, local,
    ):
        row, col, head = lax.axis_index("row"), lax.axis_index("col"), lax.axis_index("head")
        z, core = row // 2, row % 2
        x, y = head * 2 + col // 4, col % 4

        def at(x_, y_, z_, core_):
            return (z_ * 2 + core_, (x_ % 2) * 4 + y_, x_ // 2)

        peers = {
            "sib": at(x, y, z, 1 - core),
            "zp": at(x, y, (z + 1) % 8, core),
            "zm": at(x, y, (z + 7) % 8, core),
            "ap": at((x + core) % 4, (y + 1 - core) % 4, z, core),
            "am": at((x + 4 - core) % 4, (y + 3 + core) % 4, z, core),
            "bp": at((x + 1 - core) % 4, (y + core) % 4, z, core),
            "bm": at((x + 3 + core) % 4, (y + 4 - core) % 4, z, core),
            "far": at((x + 2) % 4, y, z, core),
        }
        other = at(3 - x, y, z, core)
        twin = at(x, y, z + 1 - 2 * (z % 2), core)
        near = {}
        for dr in (1, 15):
            near[f"h{dr}"] = ((row + dr) % 16, col, 1 - head)
        fellows = {k: ((row + k) % 16, col, head) for k in range(1, 16)}

        copies = {}
        order = {"n": 0}

        def remote(name, src, dst, peer):
            k = order["n"]
            order["n"] = k + 1
            c = pltpu.make_async_remote_copy(
                src_ref=src, dst_ref=dst, send_sem=send.at[k], recv_sem=recv.at[k],
                device_id=peer, device_id_type=pl.DeviceIdType.MESH,
            )
            copies[name] = c
            return c

        def go(name):
            copies[name].start()

        def got(name):
            copies[name].wait_recv()

        loads = []

        def load(src, dst):
            c = pltpu.make_async_copy(src, dst, local.at[len(loads)])
            loads.append(c)
            c.start()
            return c

        half_own = pl.ds(pl.multiple_of(core * 144, 16), 144)

        def blk(group, chain, j, part=None):
            base = (group * 8 + chain * 4 + j) * 144
            lo, n = {None: (0, 144), 0: (0, 80), 1: (80, 64)}[part]
            return wb.at[:, pl.ds(base + lo, n), :]

        def ring(tag, first, sides, own, place):
            p, m = sides
            remote(tag + "1", own(None), place(1, None), p)
            remote(tag + "2", own(None), place(2, None), m)
            remote(tag + "3a", place(1, 0), place(3, 0), p)
            remote(tag + "3b", place(2, 1), place(3, 1), m)

        ap, am, bp, bm = peers["ap"], peers["am"], peers["bp"], peers["bm"]
        ring("A", 0, (ap, am), lambda part: blk(0, 0, 0, part), lambda g, part: blk(g, 0, 0, part))
        for g in range(4):
            ring(
                f"B{g}", g, (bp, bm), lambda part, g=g: blk(g, 0, 0, part),
                lambda j, part, g=g: blk(g, 0, j, part),
            )
            src = wb.at[:, pl.ds(g * 8 * 144, 576), :]
            dst = wb.at[:, pl.ds((g * 8 + 4) * 144, 576), :]
            remote(f"S{g}", src, dst, peers["sib"])

        def slot(b, s, lo=0, n=64):
            return kvb.at[b, pl.ds(256 + s * 64 + lo, n), :]

        for b in range(3):
            own = stale_h.at[b]
            zp, zm = peers["zp"], peers["zm"]
            remote(f"R1_{b}", own, slot(b, 0), zp)
            remote(f"L1_{b}", own, slot(b, 3), zm)
            for d in (1, 2):
                remote(f"R{d + 1}_{b}", slot(b, d - 1), slot(b, d), zp)
                remote(f"L{d + 1}_{b}", slot(b, 3 + d - 1), slot(b, 3 + d), zm)
            remote(f"R4_{b}", slot(b, 2, 0, 32), slot(b, 6, 0, 32), zp)
            remote(f"L4_{b}", slot(b, 5, 32, 32), slot(b, 6, 32, 32), zm)
            remote(f"C0_{b}", own, slot(b, 7), peers["sib"])
            remote(
                f"C1_{b}", kvb.at[b, pl.ds(256, 448), :], kvb.at[b, pl.ds(256 + 512, 448), :],
                peers["sib"],
            )
            remote(
                f"X{b}", att.at[b, :, 1 - head], attr.at[b], peers["far"],
            )
        part_at = lambda p: p * 288 + core * 144
        ow_own = pl.ds(pl.multiple_of(part_at(z % 2), 16), 144)
        far0 = pl.ds(pl.multiple_of(704 + part_at(z % 2), 16), 144)
        far1 = pl.ds(pl.multiple_of(704 + part_at(1 - z % 2), 16), 144)
        remote("O", ow_h.at[ow_own, :], owb.at[far0, :], other)
        remote("OZ", owb.at[far0, :], owb.at[far0, :], twin)
        remote("OS0", owb.at[far0, :], owb.at[far0, :], peers["sib"])
        remote("OS1", owb.at[far1, :], owb.at[far1, :], peers["sib"])
        remote("Pf", xn.at[1, head], xn.at[1, head], peers["far"])
        remote("Pd", xn.at[1, head], xn.at[0, head], fellows[1])
        remote("Pu", xn.at[1, head], xn.at[2, head], fellows[15])
        remote("Pdf", xn.at[1, head], xn.at[0, head], near["h1"])
        remote("Puf", xn.at[1, head], xn.at[2, head], near["h15"])
        for k in range(1, 16):
            to = (row + k) % 16
            chunk = pl.ds(pl.multiple_of(to * 256, 256), 256)
            mine = pl.ds(pl.multiple_of(row * 256, 256), 256)
            remote(f"M{k}", part.at[:, chunk], rsb.at[k], fellows[k])
            remote(f"G{k}", redc, modp.at[:, mine], fellows[k])
            remote(f"T{k}", st, stb.at[k], fellows[k])

        c_w1 = load(fc1_h.at[half_own, :], wb.at[0, pl.ds(0, 144), :])
        c_w2 = load(fc2_h.at[half_own, :], wb.at[1, pl.ds(0, 144), :])
        c_x = load(x_h, xn.at[1, head])
        c_part = load(part_h, part)
        c_nz = load(noise_h, nz)
        c_emb = load(embed_h, emb)
        c_pos = load(pos_h, pos)
        c_wq = load(wqkv_h, wq)
        c_ow = load(ow_h, owb.at[pl.ds(64, 576), :])
        barrier = pltpu.get_barrier_semaphore()
        greet = list(fellows.values()) + list(near.values())
        greet += [peers[n] for n in ("ap", "am", "bp", "bm", "far")]
        for peer in greet:
            pl.semaphore_signal(barrier, inc=1, device_id=peer, device_id_type=pl.DeviceIdType.MESH)
        owb[pl.ds(0, 64), :] = jnp.zeros((64, D), bf)
        owb[pl.ds(640, 64), :] = jnp.zeros((64, D), bf)
        att[...] = jnp.zeros_like(att)
        acc[...] = jnp.zeros_like(acc)
        c_x.wait()
        c_part.wait()
        pl.semaphore_wait(barrier, len(greet))
        for n in ("Pf", "Pd", "Pu", "Pdf", "Puf"):
            go(n)
        for k in range(1, 16):
            go(f"M{k}")
        go("R1_0")
        go("L1_0")
        c_w1.wait()
        c_w2.wait()
        for n in ("A1", "A2", "B01", "B02"):
            go(n)
        for b in range(3):
            go(f"C0_{b}")
        go("O")
        c_nz.wait()
        c_emb.wait()
        for n in ("Pf", "Pd", "Pu", "Pdf", "Puf"):
            got(n)

        def line(d, i):
            return jnp.concatenate([xn[d, 0, :, i], xn[d, 1, :, i]], axis=-1)

        lines = [line(0, 3)] + [line(1, i) for i in range(4)] + [line(2, 0)]
        lines[0] = jnp.where(row == 0, lines[1], lines[0])
        lines[5] = jnp.where(row == 15, lines[4], lines[5])
        image = lax.broadcasted_iota(jnp.int32, (3, 4, 64), 0)

        def per_image(k):
            return jnp.where(
                image == 0, levels_s[k], jnp.where(image == 1, levels_s[k + 1], levels_s[k + 2])
            )

        keep, fuzz = per_image(0), per_image(3)
        total = jnp.zeros((3, 4, 64), f32)
        square = jnp.zeros((3, 4, 64), f32)
        for i in range(4):
            for di in range(2):
                v = 0.75 * lines[i + 1] + 0.25 * lines[i + 2 * di]
                sides = (
                    jnp.concatenate([v[:, :, :1], v[:, :, :63]], axis=-1),
                    jnp.concatenate([v[:, :, 1:], v[:, :, 63:]], axis=-1),
                )
                for dj in range(2):
                    k = 2 * di + dj
                    n = keep * (0.75 * v + 0.25 * sides[dj]) + fuzz * nz[:, i, 4 * k : 4 * k + 4, :]
                    noisy[:, i, 4 * k : 4 * k + 4, :] = n
                    total = total + n
                    square = square + n * n
        lane1 = lax.broadcasted_iota(jnp.int32, (8, 128), 1)
        both = jnp.zeros((8, 128), f32)
        for b in range(3):
            s = jnp.concatenate(
                [
                    jnp.sum(total[b], axis=1, keepdims=True),
                    jnp.sum(square[b], axis=1, keepdims=True),
                ],
                axis=0,
            )
            both = jnp.where(lane1 == b, jnp.broadcast_to(s, (8, 128)), both)
        st[...] = both
        for k in range(1, 16):
            got(f"M{k}")
        mine = pl.ds(pl.multiple_of(row * 256, 256), 256)
        piece = part[:, mine]
        for k in range(1, 16):
            piece = piece + rsb[k]
        redc[...] = piece
        modp[:, mine] = piece
        for k in range(1, 16):
            go(f"T{k}")
        for k in range(1, 16):
            go(f"G{k}")
        go("R1_1")
        go("L1_1")

        def norm(v):
            centre = jnp.mean(v, axis=-1, keepdims=True)
            v = v - centre
            spread = jnp.mean(v * v, axis=-1, keepdims=True)
            return v * lax.rsqrt(spread + 1e-06)

        def modrow(b, k):
            return modp[pl.ds(b + 4 * (k // 3), 1), pl.ds((k % 3) * D, D)]

        NT = (((1,), (1,)), ((), ()))

        def qkv(b):
            n1 = (
                norm(tok[b].reshape(256, D).astype(f32)) * (1.0 + modrow(b, 1)) + modrow(b, 0)
            ).astype(bf)
            q = lax.dot_general(n1, wq[pl.ds(0, 576), :], NT, preferred_element_type=f32)
            qb[b, :, pl.ds(0, 576)] = (q * QS).astype(bf)
            kv = lax.dot_general(n1, wq[pl.ds(576, 1152), :], NT, preferred_element_type=f32)
            kvb[b, pl.ds(0, 256), :] = kv.astype(bf)

        lane = lax.broadcasted_iota(jnp.int32, (1, 256), 1)

        def attend(b):
            def score(h):
                first = h * HD
                ks = pl.multiple_of((first // 128) * 128, 128)
                off = first - ks
                here = (lane >= off) & (lane < off + HD)
                q = qb[b, :, pl.ds(ks, 256)]
                q = jnp.where(here, q, jnp.zeros_like(q))
                return lax.dot_general(
                    q, kvb[b, :, pl.ds(ks, 256)], NT, preferred_element_type=f32
                )

            def mix(h, s):
                first = h * HD
                vs = pl.multiple_of(jnp.minimum(((576 + first) // 128) * 128, 896), 128)
                fresh, old = s[:, :256], s[:, 256:]
                top = jnp.maximum(
                    jnp.max(fresh, axis=1, keepdims=True), jnp.max(old, axis=1, keepdims=True) + 2.0
                )
                p0 = jnp.exp2(fresh - top)
                p1 = jnp.exp2(old - (top - 2.0))
                mass = jnp.sum(p0, axis=1, keepdims=True) + jnp.sum(p1, axis=1, keepdims=True)
                o = jnp.dot(
                    p0.astype(bf), kvb[b, pl.ds(0, 256), pl.ds(vs, 256)],
                    preferred_element_type=f32,
                ) + jnp.dot(
                    p1.astype(bf), kvb[b, pl.ds(256, NKEY - 256), pl.ds(vs, 256)],
                    preferred_element_type=f32,
                )
                o = (o * (1.0 / mass)).astype(bf).reshape(4, 2, 32, 256)
                voff = 576 + first - vs
                mine = (lane >= voff) & (lane < voff + HD)
                ws = pl.multiple_of(vs - 512, 128)
                att[b, :, :, :, pl.ds(ws, 256)] = jnp.where(
                    mine.reshape(1, 1, 1, 256), o, att[b, :, :, :, pl.ds(ws, 256)]
                )

            def some(i, _):
                hs = [i * UNROLL + j for j in range(UNROLL)]
                ss = [score(h) for h in hs]
                for h, s in zip(hs, ss):
                    mix(h, s)
                return 0

            lax.fori_loop(0, 8 // UNROLL, some, 0)

        def project(b):
            mine = att[b, :, head].reshape(128, 640)
            p = jnp.dot(mine, owb[pl.ds(0, 640), :], preferred_element_type=f32)
            p = p + jnp.dot(attr[b].reshape(128, 640), owb[pl.ds(640, 640), :], preferred_element_type=f32)
            t = tok[b, :, head].reshape(128, D).astype(f32)
            m = (t + modrow(b, 2) * p).astype(bf)
            mid[pl.ds(b * 128, 128), :] = m
            n = norm(m.astype(f32)) * (1.0 + modrow(b, 4)) + modrow(b, 3)
            n2[pl.ds(b * 128, 128), :] = n.astype(bf)

        def feed(first, count):
            def one(i, _):
                r = pl.ds(pl.multiple_of(first + i * 768, 256), 768)
                hid = lax.dot_general(n2[...], wb[0, r, :], NT, preferred_element_type=f32)
                hid = jax.nn.gelu(hid, approximate=True).astype(bf)
                acc[...] += jnp.dot(hid, wb[1, r, :], preferred_element_type=f32)
                return 0

            lax.fori_loop(0, count, one, 0)

        def kstep(d, b):
            got(f"R{d}_{b}")
            got(f"L{d}_{b}")
            if d < 4:
                go(f"R{d + 1}_{b}")
                go(f"L{d + 1}_{b}")

        def fwd(tag):
            got(tag + "1")
            go(tag + "3a")
            got(tag + "2")
            go(tag + "3b")

        def done(tag):
            got(tag + "3a")
            got(tag + "3b")

        kstep(1, 0)
        for k in range(1, 16):
            got(f"T{k}")
        both = st[...]
        for k in range(1, 16):
            both = both + stb[k]
        shares, gains = [], []
        for b in range(3):
            col_b = jnp.sum(jnp.where(lane1 == b, both, 0.0), axis=1, keepdims=True) / 16384.0
            centre = col_b[0:4]
            gain = lax.rsqrt(col_b[4:8] - centre * centre + 1e-05)
            shares.append(jnp.concatenate([centre] * 4, axis=0))
            gains.append(jnp.concatenate([gain] * 4, axis=0))
        whi = emb[...].astype(bf)
        wlo = (emb[...] - whi.astype(f32)).astype(bf)
        w3 = jnp.concatenate([whi, whi, wlo], axis=0)
        c_pos.wait()
        c_wq.wait()
        for b in range(3):
            for i in range(4):
                n = (noisy[b, i] - shares[b]) * gains[b]
                hi = n.astype(bf)
                lo = (n - hi.astype(f32)).astype(bf)
                e = lax.dot_general(
                    jnp.concatenate([hi, lo, hi], axis=0), w3, (((0,), (0,)), ((), ())),
                    preferred_element_type=f32,
                )
                e = (e + pos[pl.ds(i * 64, 64), :]).astype(bf)
                tok[b, i] = e.reshape(2, 32, D)
        for k in range(1, 16):
            got(f"G{k}")
        kstep(1, 1)
        qkv(0)
        kstep(2, 0)
        fwd("A")
        fwd("B0")
        for g in (1, 2):
            go(f"B{g}1")
            go(f"B{g}2")
        qkv(1)
        kstep(2, 1)
        qkv(2)
        got("O")
        go("OZ")
        go("OS0")
        kstep(3, 0)
        done("A")
        go("B31")
        go("B32")
        kstep(3, 1)
        kstep(4, 0)
        go("C1_0")
        go("R1_2")
        go("L1_2")
        got("OZ")
        go("OS1")
        got("C0_0")
        got("C1_0")
        attend(0)
        kstep(4, 1)
        go("C1_1")
        kstep(1, 2)
        done("B0")
        go("S0")
        fwd("B1")
        go("X0")
        got("C0_1")
        got("C1_1")
        kstep(2, 2)
        attend(1)
        kstep(3, 2)
        fwd("B2")
        go("X1")
        c_ow.wait()
        got("OS0")
        got("OS1")
        got("X0")
        project(0)
        kstep(4, 2)
        go("C1_2")
        fwd("B3")
        done("B1")
        go("S1")
        got("C0_2")
        got("C1_2")
        attend(2)
        go("X2")
        got("X1")
        project(1)
        done("B2")
        go("S2")
        got("X2")
        project(2)
        got("S0")
        got("S1")
        feed(0, 3)
        done("B3")
        go("S3")
        got("S2")
        feed(2304, 1)
        got("S3")
        feed(3072, 2)
        for b in range(3):
            r = pl.ds(b * 128, 128)
            out_ref[r, :] = (mid[r, :].astype(f32) + modrow(b, 5) * acc[r, :]).astype(bf)
        for c in copies.values():
            c.wait_send()

    any_spec = pl.BlockSpec(memory_space=pl.ANY)
    n_copies = 4 + 4 * 5 + 3 * 11 + 4 + 5 + 45
    return pl.pallas_call(
        kernel,
        out_shape=jax.ShapeDtypeStruct((384, D), bf),
        in_specs=[pl.BlockSpec(memory_space=pltpu.SMEM)] + [any_spec] * 10,
        out_specs=pl.BlockSpec(memory_space=pltpu.VMEM),
        scratch_shapes=[
            pltpu.VMEM((3, 2, 3, 4, 4, 32), f32),
            pltpu.VMEM((3, 4, 16, 64), f32),
            pltpu.VMEM((16, D), f32),
            pltpu.VMEM((256, D), f32),
            pltpu.VMEM((8, 4096), f32),
            pltpu.VMEM((16, 8, 256), f32),
            pltpu.VMEM((8, 256), f32),
            pltpu.VMEM((8, 4096), f32),
            pltpu.VMEM((8, 128), f32),
            pltpu.VMEM((16, 8, 128), f32),
            pltpu.VMEM((3, 4, 16, 64), f32),
            pltpu.VMEM((3, 4, 2, 32, D), bf),
            pltpu.VMEM((1728, D), bf),
            pltpu.VMEM((3, NKEY, D), bf),
            pltpu.VMEM((2, HID, D), bf),
            pltpu.VMEM((1280, D), bf),
            pltpu.VMEM((3, 256, 640), bf),
            pltpu.VMEM((3, 4, 2, 32, 640), bf),
            pltpu.VMEM((3, 4, 32, 640), bf),
            pltpu.VMEM((384, D), bf),
            pltpu.VMEM((384, D), bf),
            pltpu.VMEM((384, D), f32),
            pltpu.SemaphoreType.DMA((n_copies,)),
            pltpu.SemaphoreType.DMA((n_copies,)),
            pltpu.SemaphoreType.DMA((9,)),
        ],
        compiler_params=pltpu.CompilerParams(
            collective_id=0, has_side_effects=True, vmem_limit_bytes=64_000_000
        ),
    )(levels, x_lo, noise, embed, pos, part, stale, wqkv, ow, fc1, fc2)


def body(
    x_lo,
    noise,
    t_index,
    labels,
    stale_kv,
    embed_w,
    t_w1,
    t_w2,
    class_table,
    ada_w,
    qkv_w,
    out_w,
    fc1_w,
    fc2_w,
):
    row_index = lax.axis_index("row")
    row_count = lax.axis_size("row")
    head_index = lax.axis_index("head")
    head_count = lax.axis_size("head")
    batch = noise.shape[0]
    tile_rows = noise.shape[1]
    full_cols = noise.shape[2]
    channels = x_lo.shape[3]
    width = embed_w.shape[1]
    abar = noise_level(t_index)
    row_pos = (row_index * tile_rows + jnp.arange(tile_rows, dtype=jnp.int32)).astype(jnp.float32)
    col_pos = jnp.arange(full_cols, dtype=jnp.float32)
    pos = position_table(row_pos, col_pos, width)
    cond_part = condition(t_index, labels, t_w1, t_w2, class_table)
    cond_act = jax.nn.silu(cond_part).astype(jnp.bfloat16)
    part = jnp.dot(cond_act, ada_w, preferred_element_type=jnp.float32)
    part = part.reshape(batch, 2, 3 * width).transpose(1, 0, 2)
    part = jnp.pad(part, ((0, 0), (0, 1), (0, 4096 - 3 * width))).reshape(8, 4096)
    half = full_cols // head_count
    local_width = qkv_w.shape[2]
    stale = stale_kv.transpose(1, 2, 3, 0, 4).reshape(batch, -1, 2 * local_width)
    out = fused_block(
        jnp.concatenate([jnp.sqrt(abar), jnp.sqrt(1.0 - abar)]),
        x_lo.transpose(0, 1, 3, 2),
        noise.transpose(0, 1, 3, 2),
        embed_w,
        pos.reshape(-1, width),
        part,
        stale,
        qkv_w.transpose(1, 2, 0).reshape(3 * local_width, width),
        out_w,
        fc1_w.T,
        fc2_w.T,
    )
    return out.reshape(batch, tile_rows, half, width)


def solution(mesh):
    placed = (
        P("col", "row", "head", None),
        P("col", "row", None, None),
        P("col"),
        P("col"),
        P(None, "col", "row", None, "head"),
        P(),
        P(),
        P(None, "row"),
        P(None, "row"),
        P("row", None),
        P(None, None, "head"),
        P("head", None),
        P(None, ("col", "head")),
        P(None, ("col", "head")),
    )
    return jax.shard_map(
        body, mesh=mesh, in_specs=placed, out_specs=P("col", "row", "head", None), check_vma=False
    )
```

```python
import math

import jax
import jax.numpy as jnp
from jax import lax
from jax.experimental import pallas as pl
from jax.experimental.pallas import tpu as pltpu
from jax.sharding import PartitionSpec as P

HD = 72
TSTEPS = 1000


def fused_block(t_index, labels, x_lo, noise, embed, tw1, tw2, table, ada, stale, wqkv, ow, fc1, fc2):
    D = 1152
    L2E = 1.4426950408889634
    QS = L2E / math.sqrt(HD)
    bf, f32 = jnp.bfloat16, jnp.float32
    NKEY = 256 + 15 * 64
    HID = 4608
    UNROLL = 2
    EARLY = 256 + 9 * 64

    def kernel(
        t_s, label_s, x_h, noise_h, embed_h, tw1_h, tw2_h, table_h, ada_h, stale_h, wqkv_h, ow_h, fc1_h,
        fc2_h, out_ref, xn, nz, emb, pos, tw1, tw2, table, ada, skv, kown, att1, mass1, part, rsb, both_ref, gs, modp, noisy,
        tok, wq, kvb, wb, owb, qb, att, attr, n2, mid, acc, send, recv, local,
    ):
        row, col, head = lax.axis_index("row"), lax.axis_index("col"), lax.axis_index("head")
        z, core = row // 2, row % 2
        x, y = head * 2 + col // 4, col % 4

        def at(x_, y_, z_, core_):
            return (z_ * 2 + core_, (x_ % 2) * 4 + y_, x_ // 2)

        peers = {
            "sib": at(x, y, z, 1 - core),
            "zp": at(x, y, (z + 1) % 8, core),
            "zm": at(x, y, (z + 7) % 8, core),
            "ap": at((x + core) % 4, (y + 1 - core) % 4, z, core),
            "am": at((x + 4 - core) % 4, (y + 3 + core) % 4, z, core),
            "bp": at((x + 1 - core) % 4, (y + core) % 4, z, core),
            "bm": at((x + 3 + core) % 4, (y + 4 - core) % 4, z, core),
            "far": at((x + 2) % 4, y, z, core),
        }
        other = at(3 - x, y, z, core)
        twin = at(x, y, z + 1 - 2 * (z % 2), core)
        near = {}
        for dr in (1, 15):
            near[f"h{dr}"] = ((row + dr) % 16, col, 1 - head)
        fellows = {k: ((row + k) % 16, col, head) for k in range(1, 16)}

        copies = {}
        order = {"n": 0}

        def remote(name, src, dst, peer):
            k = order["n"]
            order["n"] = k + 1
            c = pltpu.make_async_remote_copy(
                src_ref=src, dst_ref=dst, send_sem=send.at[k], recv_sem=recv.at[k],
                device_id=peer, device_id_type=pl.DeviceIdType.MESH,
            )
            copies[name] = c
            return c

        def go(name):
            copies[name].start()

        def got(name):
            copies[name].wait_recv()

        loads = []

        def load(src, dst):
            c = pltpu.make_async_copy(src, dst, local.at[len(loads)])
            loads.append(c)
            c.start()
            return c

        SIZE, PLUS, LIFT = {"": 112, "E": 32}, {"": 64, "E": 16}, {"": 0, "E": 448}

        def blk(kind, group, j, part=None):
            lo, n = {
                None: (0, SIZE[kind]), 0: (0, PLUS[kind]), 1: (PLUS[kind], SIZE[kind] - PLUS[kind])
            }[part]
            return wb.at[:, pl.ds(group * 1152 + LIFT[kind] + j * SIZE[kind] + lo, n), :]

        def ring(tag, sides, place):
            p, m = sides
            remote(tag + "1", place(0, None), place(1, None), p)
            remote(tag + "2", place(0, None), place(2, None), m)
            remote(tag + "3a", place(1, 0), place(3, 0), p)
            remote(tag + "3b", place(2, 1), place(3, 1), m)

        along = {
            "A": (peers["ap"], peers["am"]),
            "B": (peers["bp"], peers["bm"]),
            "EA": (at((x + 1) % 4, y, z, core), at((x + 3) % 4, y, z, core)),
            "EB": (at(x, (y + 1) % 4, z, core), at(x, (y + 3) % 4, z, core)),
        }
        for kind in ("", "E"):
            ring(kind + "A", along[kind + "A"], lambda g, part, kind=kind: blk(kind, g, 0, part))
            for g in range(4):
                ring(
                    f"{kind}B{g}", along[kind + "B"],
                    lambda j, part, g=g, kind=kind: blk(kind, g, j, part),
                )
        for name, lo, n in [(f"S{g}", g * 1152, 576) for g in range(3)] + [
            ("S3m", 3456, 336), ("S3e", 3904, 96), ("S3mz", 3792, 112), ("S3ez", 4000, 32)
        ]:
            remote(name, wb.at[:, pl.ds(lo, n), :], wb.at[:, pl.ds(lo + 576, n), :], peers["sib"])

        def slot(b, s, lo=0, n=64):
            return kvb.at[b, pl.ds(256 + s * 64 + lo, n), :]

        for b in range(3):
            own = kown.at[b]
            zp, zm = peers["zp"], peers["zm"]
            right, left = (0, 2, 9), (1, 3, 10)
            remote(f"R1_{b}", own, slot(b, 0), zp)
            remote(f"L1_{b}", own, slot(b, 1), zm)
            for d in (1, 2):
                remote(f"R{d + 1}_{b}", slot(b, right[d - 1]), slot(b, right[d]), zp)
                remote(f"L{d + 1}_{b}", slot(b, left[d - 1]), slot(b, left[d]), zm)
            remote(f"R4_{b}", slot(b, 9, 0, 32), slot(b, 11, 0, 32), zp)
            remote(f"L4_{b}", slot(b, 10, 32, 32), slot(b, 11, 32, 32), zm)
            remote(f"C0_{b}", own, slot(b, 4), peers["sib"])
            remote(f"C1_{b}", slot(b, 0, 0, 256), slot(b, 5, 0, 256), peers["sib"])
            remote(f"C2_{b}", slot(b, 9, 0, 192), slot(b, 12, 0, 192), peers["sib"])
            remote(
                f"X{b}", att.at[b, :, 1 - head], attr.at[b], peers["far"],
            )
        part_at = lambda p: p * 288 + core * 144
        ow_own = pl.ds(pl.multiple_of(part_at(z % 2), 16), 144)
        far0 = pl.ds(pl.multiple_of(704 + part_at(z % 2), 16), 144)
        far1 = pl.ds(pl.multiple_of(704 + part_at(1 - z % 2), 16), 144)
        remote("O", ow_h.at[ow_own, :], owb.at[far0, :], other)
        remote("OZ", owb.at[far0, :], owb.at[far0, :], twin)
        remote("OS0", owb.at[far0, :], owb.at[far0, :], peers["sib"])
        remote("OS1", owb.at[far1, :], owb.at[far1, :], peers["sib"])
        remote("Pf", xn.at[1, head], xn.at[1, head], peers["far"])
        remote("Pd", xn.at[1, head], xn.at[0, head], fellows[1])
        remote("Pu", xn.at[1, head], xn.at[2, head], fellows[15])
        remote("Pdf", xn.at[1, head], xn.at[0, head], near["h1"])
        remote("Puf", xn.at[1, head], xn.at[2, head], near["h15"])
        for k in range(1, 16):
            to = (row + k) % 16
            chunk = pl.ds(pl.multiple_of(to * 256, 256), 256)
            remote(f"M{k}", part.at[:, chunk], rsb.at[k], fellows[k])
            remote(f"G{k}", both_ref, gs.at[row], fellows[k])

        c_w = []
        for kind, lo in (("", 0), ("E", 112)):
            rows = pl.ds(pl.multiple_of(core * 144 + lo, 16), SIZE[kind])
            for k, w_h in enumerate((fc1_h, fc2_h)):
                c_w.append(load(w_h.at[rows, :], wb.at[k, pl.ds(LIFT[kind], SIZE[kind]), :]))
        c_x = load(x_h, xn.at[1, head])
        c_tw1 = load(tw1_h, tw1)
        c_tw2 = load(tw2_h, tw2)
        c_table = load(table_h, table)
        c_ada = load(ada_h, ada)
        c_skv = load(stale_h, skv)
        c_nz = load(noise_h, nz)
        c_emb = load(embed_h, emb)
        c_wq = load(wqkv_h, wq)
        c_ow = load(ow_h, owb.at[pl.ds(64, 576), :])
        barrier = pltpu.get_barrier_semaphore()
        greet = list(fellows.values()) + list(near.values())
        greet += [peers[n] for n in ("ap", "am", "bp", "bm", "far")]
        for peer in greet:
            pl.semaphore_signal(barrier, inc=1, device_id=peer, device_id_type=pl.DeviceIdType.MESH)
        owb[pl.ds(0, 64), :] = jnp.zeros((64, D), bf)
        owb[pl.ds(640, 64), :] = jnp.zeros((64, D), bf)
        att[...] = jnp.zeros_like(att)
        att1[...] = jnp.zeros_like(att1)
        mass1[...] = jnp.zeros_like(mass1)
        acc[...] = jnp.zeros_like(acc)
        c_skv.wait()
        for b in range(3):
            kown[b] = jnp.concatenate([skv[0, b], skv[1, b]], axis=-1).reshape(64, D)
        def by_image(values, shape):
            r = lax.broadcasted_iota(jnp.int32, shape, 0)
            return jnp.where(r == 0, values[0], jnp.where(r == 1, values[1], values[2]))

        ts = [t_s[b] for b in range(3)]
        k128 = lax.broadcasted_iota(jnp.int32, (8, 128), 1).astype(f32)
        angles = by_image(ts, (8, 128)).astype(f32) * jnp.exp(-math.log(10000.0) * k128 / 128)
        feats = jnp.concatenate([jnp.cos(angles), jnp.sin(angles)], axis=1).astype(bf)
        c_tw1.wait()
        hid = jnp.dot(feats, tw1[...], preferred_element_type=f32)
        hid = (hid * jax.nn.sigmoid(hid)).astype(bf)
        c_tw2.wait()
        c_table.wait()
        NT = (((1,), (1,)), ((), ()))
        kinds = lax.broadcasted_iota(jnp.int32, (8, 1001), 1)
        picked = kinds == by_image([label_s[b] for b in range(3)], (8, 1001))
        cond = lax.dot_general(hid, tw2[...], NT, preferred_element_type=f32)
        cond = cond + lax.dot_general(
            picked.astype(f32).astype(bf), table[...], NT, preferred_element_type=f32
        )
        cond = (cond * jax.nn.sigmoid(cond)).astype(bf)
        c_ada.wait()
        for k in range(2):
            first = jnp.dot(cond, ada[:, pl.ds(k * 3 * D, 3 * D)], preferred_element_type=f32)
            part[pl.ds(4 * k, 4), pl.ds(0, 3 * D)] = first[0:4]
        steps = lax.broadcasted_iota(jnp.int32, (8, TSTEPS), 1)
        betas = 0.0001 + (0.02 - 0.0001) * steps.astype(f32) / (TSTEPS - 1)
        logs = jnp.where(steps <= by_image(ts, (8, TSTEPS)), jnp.log(1.0 - betas), 0.0)
        abar = jnp.exp(jnp.sum(logs, axis=1, keepdims=True))

        def wide(column):
            return jnp.stack([jnp.broadcast_to(column[b : b + 1], (4, 64)) for b in range(3)])

        keep, fuzz = wide(jnp.sqrt(abar)), wide(jnp.sqrt(1.0 - abar))

        def waves(n, start):
            place = (lax.broadcasted_iota(jnp.int32, (n, D // 4), 0) + start).astype(f32)
            k = lax.broadcasted_iota(jnp.int32, (n, D // 4), 1).astype(f32)
            args = place * jnp.exp(-math.log(10000.0) * k / (D // 4))
            return jnp.concatenate([jnp.sin(args), jnp.cos(args)], axis=1)

        rp, cp = waves(8, row * 4), waves(64, 0)
        for i in range(4):
            pos[pl.ds(i * 64, 64), :] = jnp.concatenate(
                [jnp.broadcast_to(rp[i : i + 1], (64, D // 2)), cp], axis=1
            )
        c_x.wait()
        pl.semaphore_wait(barrier, len(greet))
        for n in ("Pf", "Pd", "Pu", "Pdf", "Puf"):
            go(n)
        for k in range(1, 16):
            go(f"M{k}")
        go("R1_0")
        go("L1_0")
        for c in c_w:
            c.wait()
        for n in ("A1", "A2", "EA1", "EA2", "B01", "B02", "EB01", "EB02"):
            go(n)
        for b in range(3):
            go(f"C0_{b}")
        c_nz.wait()
        c_emb.wait()
        for n in ("Pf", "Pd", "Pu", "Pdf", "Puf"):
            got(n)

        def line(d, i):
            return jnp.concatenate([xn[d, 0, :, i], xn[d, 1, :, i]], axis=-1)

        lines = [line(0, 3)] + [line(1, i) for i in range(4)] + [line(2, 0)]
        lines[0] = jnp.where(row == 0, lines[1], lines[0])
        lines[5] = jnp.where(row == 15, lines[4], lines[5])
        total = jnp.zeros((3, 4, 64), f32)
        square = jnp.zeros((3, 4, 64), f32)
        for i in range(4):
            for di in range(2):
                v = 0.75 * lines[i + 1] + 0.25 * lines[i + 2 * di]
                sides = (
                    jnp.concatenate([v[:, :, :1], v[:, :, :63]], axis=-1),
                    jnp.concatenate([v[:, :, 1:], v[:, :, 63:]], axis=-1),
                )
                for dj in range(2):
                    k = 2 * di + dj
                    n = keep * (0.75 * v + 0.25 * sides[dj]) + fuzz * nz[:, i, 4 * k : 4 * k + 4, :]
                    noisy[:, i, 4 * k : 4 * k + 4, :] = n
                    total = total + n
                    square = square + n * n
        lane1 = lax.broadcasted_iota(jnp.int32, (8, 128), 1)
        both = jnp.zeros((8, 128), f32)
        for b in range(3):
            s = jnp.concatenate(
                [
                    jnp.sum(total[b], axis=1, keepdims=True),
                    jnp.sum(square[b], axis=1, keepdims=True),
                ],
                axis=0,
            )
            both = jnp.where(lane1 == b, jnp.broadcast_to(s, (8, 128)), both)
        both_ref[:, pl.ds(256, 128)] = both
        for k in range(1, 16):
            got(f"M{k}")
        mine = pl.ds(pl.multiple_of(row * 256, 256), 256)
        piece = part[:, mine]
        for k in range(1, 16):
            piece = piece + rsb[k]
        both_ref[:, pl.ds(0, 256)] = piece
        gs[row] = jnp.concatenate([piece, both], axis=1)
        for k in range(1, 16):
            go(f"G{k}")
        for b in (1, 2):
            go(f"R1_{b}")
            go(f"L1_{b}")

        def norm(v):
            centre = jnp.mean(v, axis=-1, keepdims=True)
            v = v - centre
            spread = jnp.mean(v * v, axis=-1, keepdims=True)
            return v * lax.rsqrt(spread + 1e-06)

        def modrow(b, k):
            return modp[pl.ds(b + 4 * (k // 3), 1), pl.ds((k % 3) * D, D)]

        def qkv(b):
            n1 = (
                norm(tok[b].reshape(256, D).astype(f32)) * (1.0 + modrow(b, 1)) + modrow(b, 0)
            ).astype(bf)
            q = lax.dot_general(n1, wq[pl.ds(0, 576), :], NT, preferred_element_type=f32)
            qb[b, :, pl.ds(0, 576)] = (q * QS).astype(bf)
            kv = lax.dot_general(n1, wq[pl.ds(576, 1152), :], NT, preferred_element_type=f32)
            kvb[b, pl.ds(0, 256), :] = kv.astype(bf)

        lane = lax.broadcasted_iota(jnp.int32, (1, 256), 1)

        lane128 = lax.broadcasted_iota(jnp.int32, (1, 128), 1)

        def attend(b, late):
            keys = pl.ds(EARLY, NKEY - EARLY) if late else pl.ds(0, EARLY)

            def score(h):
                first = h * HD
                ks = pl.multiple_of((first // 128) * 128, 128)
                off = first - ks
                here = (lane >= off) & (lane < off + HD)
                q = qb[b, :, pl.ds(ks, 256)]
                q = jnp.where(here, q, jnp.zeros_like(q))
                return lax.dot_general(
                    q, kvb[b, keys, pl.ds(ks, 256)], NT, preferred_element_type=f32
                )

            def mix(h, s):
                first = h * HD
                vs = pl.multiple_of(jnp.minimum(((576 + first) // 128) * 128, 896), 128)
                voff = 576 + first - vs
                mine = (lane >= voff) & (lane < voff + HD)
                cols = pl.ds(pl.multiple_of(vs - 512, 128), 256)
                chosen = lane128 == h
                if late:
                    top = jnp.max(s, axis=1, keepdims=True) + 2.0
                    before = jnp.sum(jnp.where(chosen, mass1[b], 0.0), axis=1, keepdims=True)
                    top = jnp.maximum(top, before)
                    p = jnp.exp2(s - (top - 2.0))
                    kept = jnp.exp2(before - top)
                    mass = jnp.sum(p, axis=1, keepdims=True) + kept
                    o = jnp.dot(p.astype(bf), kvb[b, keys, pl.ds(vs, 256)], preferred_element_type=f32)
                    o = (o + kept * att1[b, :, cols]) * (1.0 / mass)
                    o = o.astype(bf).reshape(4, 2, 32, 256)
                    att[b, :, :, :, cols] = jnp.where(
                        mine.reshape(1, 1, 1, 256), o, att[b, :, :, :, cols]
                    )
                    return
                fresh, old = s[:, :256], s[:, 256:]
                top = jnp.maximum(
                    jnp.max(fresh, axis=1, keepdims=True), jnp.max(old, axis=1, keepdims=True) + 2.0
                )
                p0 = jnp.exp2(fresh - top)
                p1 = jnp.exp2(old - (top - 2.0))
                mass = jnp.sum(p0, axis=1, keepdims=True) + jnp.sum(p1, axis=1, keepdims=True)
                o = jnp.dot(
                    p0.astype(bf), kvb[b, pl.ds(0, 256), pl.ds(vs, 256)],
                    preferred_element_type=f32,
                ) + jnp.dot(
                    p1.astype(bf), kvb[b, pl.ds(256, EARLY - 256), pl.ds(vs, 256)],
                    preferred_element_type=f32,
                )
                att1[b, :, cols] = jnp.where(mine, o * (1.0 / mass), att1[b, :, cols])
                mass1[b] = jnp.where(chosen, top + jnp.log2(mass), mass1[b])

            def some(i, _):
                hs = [i * UNROLL + j for j in range(UNROLL)]
                ss = [score(h) for h in hs]
                for h, s in zip(hs, ss):
                    mix(h, s)
                return 0

            lax.fori_loop(0, 8 // UNROLL, some, 0)

        def project(b):
            mine = att[b, :, head].reshape(128, 640)
            p = jnp.dot(mine, owb[pl.ds(0, 640), :], preferred_element_type=f32)
            p = p + jnp.dot(attr[b].reshape(128, 640), owb[pl.ds(640, 640), :], preferred_element_type=f32)
            t = tok[b, :, head].reshape(128, D).astype(f32)
            m = (t + modrow(b, 2) * p).astype(bf)
            mid[pl.ds(b * 128, 128), :] = m
            n = norm(m.astype(f32)) * (1.0 + modrow(b, 4)) + modrow(b, 3)
            n2[pl.ds(b * 128, 128), :] = n.astype(bf)

        def feed(first, count):
            def one(i, _):
                r = pl.ds(pl.multiple_of(first + i * 768, 256), 768)
                hid = lax.dot_general(n2[...], wb[0, r, :], NT, preferred_element_type=f32)
                hid = jax.nn.gelu(hid, approximate=True).astype(bf)
                acc[...] += jnp.dot(hid, wb[1, r, :], preferred_element_type=f32)
                return 0

            lax.fori_loop(0, count, one, 0)

        def kstep(d, b):
            got(f"R{d}_{b}")
            got(f"L{d}_{b}")
            if d < 4:
                go(f"R{d + 1}_{b}")
                go(f"L{d + 1}_{b}")

        def fwd(tag):
            got(tag + "1")
            go(tag + "3a")
            got(tag + "2")
            go(tag + "3b")

        def done(tag):
            got(tag + "3a")
            got(tag + "3b")

        kstep(1, 0)
        for k in range(1, 16):
            got(f"G{k}")
        both = jnp.zeros((8, 128), f32)
        for r in range(16):
            both = both + gs[r, :, pl.ds(256, 128)]
            modp[:, pl.ds(r * 256, 256)] = gs[r, :, pl.ds(0, 256)]
        shares, gains = [], []
        for b in range(3):
            col_b = jnp.sum(jnp.where(lane1 == b, both, 0.0), axis=1, keepdims=True) / 16384.0
            centre = col_b[0:4]
            gain = lax.rsqrt(col_b[4:8] - centre * centre + 1e-05)
            shares.append(jnp.concatenate([centre] * 4, axis=0))
            gains.append(jnp.concatenate([gain] * 4, axis=0))
        whi = emb[...].astype(bf)
        wlo = (emb[...] - whi.astype(f32)).astype(bf)
        w3 = jnp.concatenate([whi, whi, wlo], axis=0)
        c_wq.wait()
        for b in range(3):
            for i in range(4):
                n = (noisy[b, i] - shares[b]) * gains[b]
                hi = n.astype(bf)
                lo = (n - hi.astype(f32)).astype(bf)
                e = lax.dot_general(
                    jnp.concatenate([hi, lo, hi], axis=0), w3, (((0,), (0,)), ((), ())),
                    preferred_element_type=f32,
                )
                e = (e + pos[pl.ds(i * 64, 64), :]).astype(bf)
                tok[b, i] = e.reshape(2, 32, D)
        def both_kinds(act, tag):
            act(tag)
            act("E" + tag)

        def begin(tag):
            go(tag + "1")
            go(tag + "2")

        both_kinds(fwd, "A")
        for g in (1, 2):
            both_kinds(begin, f"B{g}")
        go("O")
        kstep(1, 1)
        qkv(0)
        kstep(1, 2)
        qkv(1)
        kstep(2, 0)
        go("C1_0")
        both_kinds(fwd, "B0")
        qkv(2)
        kstep(2, 1)
        go("C1_1")
        got("C0_0")
        got("C1_0")
        attend(0, False)
        kstep(2, 2)
        go("C1_2")
        both_kinds(done, "A")
        both_kinds(begin, "B3")
        got("C0_1")
        got("C1_1")
        kstep(3, 0)
        attend(1, False)
        kstep(3, 1)
        got("C0_2")
        got("C1_2")
        got("O")
        go("OS0")
        attend(2, False)
        kstep(3, 2)
        kstep(4, 0)
        go("C2_0")
        both_kinds(fwd, "B1")
        kstep(4, 1)
        go("C2_1")
        got("C2_0")
        attend(0, True)
        go("X0")
        kstep(4, 2)
        go("C2_2")
        go("OZ")
        got("C2_1")
        attend(1, True)
        go("X1")
        both_kinds(done, "B0")
        go("S0")
        got("C2_2")
        attend(2, True)
        go("X2")
        both_kinds(fwd, "B2")
        got("OZ")
        go("OS1")
        c_ow.wait()
        got("OS0")
        got("X0")
        got("OS1")
        project(0)
        both_kinds(fwd, "B3")
        go("S3m")
        go("S3e")
        got("X1")
        project(1)
        got("X2")
        project(2)
        got("S0")
        feed(0, 1)
        both_kinds(done, "B1")
        go("S1")
        both_kinds(done, "B2")
        go("S2")
        got("S1")
        feed(768, 2)
        both_kinds(done, "B3")
        go("S3mz")
        go("S3ez")
        got("S2")
        feed(2304, 1)
        got("S3m")
        feed(3072, 1)
        got("S3e")
        got("S3mz")
        got("S3ez")
        feed(3840, 1)
        for b in range(3):
            r = pl.ds(b * 128, 128)
            out_ref[r, :] = (mid[r, :].astype(f32) + modrow(b, 5) * acc[r, :]).astype(bf)
        for c in copies.values():
            c.wait_send()

    any_spec = pl.BlockSpec(memory_space=pl.ANY)
    n_copies = 2 * 20 + 7 + 3 * 12 + 4 + 5 + 30
    return pl.pallas_call(
        kernel,
        out_shape=jax.ShapeDtypeStruct((384, D), bf),
        in_specs=[pl.BlockSpec(memory_space=pltpu.SMEM)] * 2 + [any_spec] * 12,
        out_specs=pl.BlockSpec(memory_space=pltpu.VMEM),
        scratch_shapes=[
            pltpu.VMEM((3, 2, 3, 4, 4, 32), f32),
            pltpu.VMEM((3, 4, 16, 64), f32),
            pltpu.VMEM((16, D), f32),
            pltpu.VMEM((256, D), f32),
            pltpu.VMEM((256, D), bf),
            pltpu.VMEM((72, D), bf),
            pltpu.VMEM((72, 1001), bf),
            pltpu.VMEM((72, 6 * D), bf),
            pltpu.VMEM((2, 3, 2, 32, 576), bf),
            pltpu.VMEM((3, 64, D), bf),
            pltpu.VMEM((3, 256, 640), f32),
            pltpu.VMEM((3, 256, 128), f32),
            pltpu.VMEM((8, 4096), f32),
            pltpu.VMEM((16, 8, 256), f32),
            pltpu.VMEM((8, 384), f32),
            pltpu.VMEM((16, 8, 384), f32),
            pltpu.VMEM((8, 4096), f32),
            pltpu.VMEM((3, 4, 16, 64), f32),
            pltpu.VMEM((3, 4, 2, 32, D), bf),
            pltpu.VMEM((1728, D), bf),
            pltpu.VMEM((3, NKEY, D), bf),
            pltpu.VMEM((2, HID, D), bf),
            pltpu.VMEM((1280, D), bf),
            pltpu.VMEM((3, 256, 640), bf),
            pltpu.VMEM((3, 4, 2, 32, 640), bf),
            pltpu.VMEM((3, 4, 32, 640), bf),
            pltpu.VMEM((384, D), bf),
            pltpu.VMEM((384, D), bf),
            pltpu.VMEM((384, D), f32),
            pltpu.SemaphoreType.DMA((n_copies,)),
            pltpu.SemaphoreType.DMA((n_copies,)),
            pltpu.SemaphoreType.DMA((14,)),
        ],
        compiler_params=pltpu.CompilerParams(
            collective_id=0, has_side_effects=True, vmem_limit_bytes=64_000_000
        ),
    )(t_index, labels, x_lo, noise, embed, tw1, tw2, table, ada, stale, wqkv, ow, fc1, fc2)


def body(
    x_lo,
    noise,
    t_index,
    labels,
    stale_kv,
    embed_w,
    t_w1,
    t_w2,
    class_table,
    ada_w,
    qkv_w,
    out_w,
    fc1_w,
    fc2_w,
):
    head_count = lax.axis_size("head")
    tile_rows, full_cols = noise.shape[1], noise.shape[2]
    batch, width = noise.shape[0], embed_w.shape[1]
    half = full_cols // head_count
    local_width = qkv_w.shape[2]
    out = fused_block(
        t_index,
        labels,
        x_lo.transpose(0, 1, 3, 2),
        noise.transpose(0, 1, 3, 2),
        embed_w,
        t_w1,
        t_w2.T,
        class_table.T,
        ada_w,
        stale_kv,
        qkv_w.transpose(1, 2, 0).reshape(3 * local_width, width),
        out_w,
        fc1_w.T,
        fc2_w.T,
    )
    return out.reshape(batch, tile_rows, half, width)


def solution(mesh):
    placed = (
        P("col", "row", "head", None),
        P("col", "row", None, None),
        P("col"),
        P("col"),
        P(None, "col", "row", None, "head"),
        P(),
        P(),
        P(None, "row"),
        P(None, "row"),
        P("row", None),
        P(None, None, "head"),
        P("head", None),
        P(None, ("col", "head")),
        P(None, ("col", "head")),
    )
    return jax.shard_map(
        body, mesh=mesh, in_specs=placed, out_specs=P("col", "row", "head", None), check_vma=False
    )
```

```python
import math

import jax
import jax.numpy as jnp
from jax import lax
from jax.experimental import pallas as pl
from jax.experimental.pallas import tpu as pltpu
from jax.sharding import PartitionSpec as P

HD = 72
TSTEPS = 1000


def fused_block(t_index, labels, x_lo, noise, embed, tw1, tw2, table, ada, stale, wqkv, ow, fc1, fc2):
    D = 1152
    L2E = 1.4426950408889634
    QS = L2E / math.sqrt(HD)
    bf, f32 = jnp.bfloat16, jnp.float32
    NKEY = 256 + 15 * 64
    HID = 4608
    UNROLL = 2
    EARLY = 256 + 9 * 64

    def kernel(
        t_s, label_s, x_h, noise_h, embed_h, tw1_h, tw2_h, table_h, ada_h, stale_h, wqkv_h, ow_h, fc1_h,
        fc2_h, out_ref, xn, nz, emb, pos, tw1, tw2, table, ada, skv, kown, att1, mass1, part, pieces, rsb, both_ref, gs, modp, noisy,
        tok, wq, kvb, wb, owb, qb, att, attr, n2, mid, acc, outb, send, recv, local,
    ):
        row, col, head = lax.axis_index("row"), lax.axis_index("col"), lax.axis_index("head")
        z, core = row // 2, row % 2
        x, y = head * 2 + col // 4, col % 4

        def at(x_, y_, z_, core_):
            return (z_ * 2 + core_, (x_ % 2) * 4 + y_, x_ // 2)

        peers = {
            "sib": at(x, y, z, 1 - core),
            "zp": at(x, y, (z + 1) % 8, core),
            "zm": at(x, y, (z + 7) % 8, core),
            "ap": at((x + core) % 4, (y + 1 - core) % 4, z, core),
            "am": at((x + 4 - core) % 4, (y + 3 + core) % 4, z, core),
            "bp": at((x + 1 - core) % 4, (y + core) % 4, z, core),
            "bm": at((x + 3 + core) % 4, (y + 4 - core) % 4, z, core),
            "far": at((x + 2) % 4, y, z, core),
        }
        other = at(3 - x, y, z, core)
        twin = at(x, y, z + 1 - 2 * (z % 2), core)
        near = {}
        for dr in (1, 15):
            near[f"h{dr}"] = ((row + dr) % 16, col, 1 - head)
        fellows = {k: ((row + k) % 16, col, head) for k in range(1, 16)}

        copies = {}
        order = {"n": 0}

        def remote(name, src, dst, peer):
            k = order["n"]
            order["n"] = k + 1
            c = pltpu.make_async_remote_copy(
                src_ref=src, dst_ref=dst, send_sem=send.at[k], recv_sem=recv.at[k],
                device_id=peer, device_id_type=pl.DeviceIdType.MESH,
            )
            copies[name] = c
            return c

        def go(name):
            copies[name].start()

        def got(name):
            copies[name].wait_recv()

        loads = []

        def load(src, dst):
            c = pltpu.make_async_copy(src, dst, local.at[len(loads)])
            loads.append(c)
            c.start()
            return c

        SIZE, PLUS = {"": 112, "E": 32}, {"": 64, "E": 16}

        def blk(kind, group, j, part=None):
            lo, n = {
                None: (0, SIZE[kind]), 0: (0, PLUS[kind]), 1: (PLUS[kind], SIZE[kind] - PLUS[kind])
            }[part]
            if j < 3:
                base = group * 864 + (336 if kind else 0) + j * SIZE[kind]
            else:
                base = 3456 + group * 288 + (112 if kind else 0)
            return wb.at[:, pl.ds(base + lo, n), :]

        def ring(tag, sides, place):
            p, m = sides
            remote(tag + "1", place(0, None), place(1, None), p)
            remote(tag + "2", place(0, None), place(2, None), m)
            remote(tag + "3a", place(1, 0), place(3, 0), p)
            remote(tag + "3b", place(2, 1), place(3, 1), m)

        along = {
            "A": (peers["ap"], peers["am"]),
            "B": (peers["bp"], peers["bm"]),
            "EA": (at((x + 1) % 4, y, z, core), at((x + 3) % 4, y, z, core)),
            "EB": (at(x, (y + 1) % 4, z, core), at(x, (y + 3) % 4, z, core)),
        }
        for kind in ("", "E"):
            ring(kind + "A", along[kind + "A"], lambda g, part, kind=kind: blk(kind, g, 0, part))
            for g in range(4):
                ring(
                    f"{kind}B{g}", along[kind + "B"],
                    lambda j, part, g=g, kind=kind: blk(kind, g, j, part),
                )
        for g in range(4):
            for name, lo, n in ((f"S{g}a", g * 864, 432), (f"S{g}b", 3456 + g * 288, 144)):
                remote(
                    name, wb.at[:, pl.ds(lo, n), :], wb.at[:, pl.ds(lo + n, n), :], peers["sib"]
                )

        def slot(b, s, lo=0, n=64):
            return kvb.at[b, pl.ds(256 + s * 64 + lo, n), :]

        for b in range(3):
            own = kown.at[b]
            zp, zm = peers["zp"], peers["zm"]
            right, left = (0, 2, 9), (1, 3, 10)
            remote(f"R1_{b}", own, slot(b, 0), zp)
            remote(f"L1_{b}", own, slot(b, 1), zm)
            for d in (1, 2):
                remote(f"R{d + 1}_{b}", slot(b, right[d - 1]), slot(b, right[d]), zp)
                remote(f"L{d + 1}_{b}", slot(b, left[d - 1]), slot(b, left[d]), zm)
            remote(f"R4_{b}", slot(b, 9, 0, 32), slot(b, 11, 0, 32), zp)
            remote(f"L4_{b}", slot(b, 10, 32, 32), slot(b, 11, 32, 32), zm)
            remote(f"C0_{b}", own, slot(b, 4), peers["sib"])
            remote(f"C1_{b}", slot(b, 0, 0, 256), slot(b, 5, 0, 256), peers["sib"])
            remote(f"C2_{b}", slot(b, 9, 0, 192), slot(b, 12, 0, 192), peers["sib"])
            remote(
                f"X{b}", att.at[b, :, 1 - head], attr.at[b], peers["far"],
            )
        part_at = lambda p: p * 288 + core * 144
        ow_own = pl.ds(pl.multiple_of(part_at(z % 2), 16), 144)
        far0 = pl.ds(pl.multiple_of(704 + part_at(z % 2), 16), 144)
        far1 = pl.ds(pl.multiple_of(704 + part_at(1 - z % 2), 16), 144)
        remote("O", ow_h.at[ow_own, :], owb.at[far0, :], other)
        remote("OZ", owb.at[far0, :], owb.at[far0, :], twin)
        remote("OS0", owb.at[far0, :], owb.at[far0, :], peers["sib"])
        remote("OS1", owb.at[far1, :], owb.at[far1, :], peers["sib"])
        remote("Pf", xn.at[1, head], xn.at[1, head], peers["far"])
        remote("Pd", xn.at[1, head], xn.at[0, head], fellows[1])
        remote("Pu", xn.at[1, head], xn.at[2, head], fellows[15])
        remote("Pdf", xn.at[1, head], xn.at[0, head], near["h1"])
        remote("Puf", xn.at[1, head], xn.at[2, head], near["h15"])
        shared = {}
        for tag in "MG":
            shared[tag] = order["n"]
            order["n"] += 1
        to_all = {"M": [], "G": []}
        for k in range(1, 16):
            to = (row + k) % 16
            chunk = pl.ds(pl.multiple_of(to * 128, 128), 128)
            for tag, src, dst in (
                ("M", pieces.at[:, chunk], rsb.at[k]), ("G", both_ref, gs.at[k])
            ):
                to_all[tag].append(
                    pltpu.make_async_remote_copy(
                        src_ref=src, dst_ref=dst, send_sem=send.at[shared[tag]],
                        recv_sem=recv.at[shared[tag]], device_id=fellows[k],
                        device_id_type=pl.DeviceIdType.MESH,
                    )
                )

        def all15(tag):
            buf = {"M": rsb, "G": gs}[tag].at[pl.ds(1, 15)]
            return pltpu.make_async_remote_copy(
                src_ref=buf, dst_ref=buf, send_sem=send.at[shared[tag]],
                recv_sem=recv.at[shared[tag]], device_id=fellows[1],
                device_id_type=pl.DeviceIdType.MESH,
            )

        c_w = []
        for kind, lo in (("", 0), ("E", 112)):
            rows = pl.ds(pl.multiple_of(core * 144 + lo, 16), SIZE[kind])
            for k, w_h in enumerate((fc1_h, fc2_h)):
                c_w.append(load(w_h.at[rows, :], wb.at[k, pl.ds(336 if kind else 0, SIZE[kind]), :]))
        c_x = load(x_h, xn.at[1, head])
        c_tw1 = load(tw1_h, tw1)
        c_tw2 = load(tw2_h, tw2)
        c_table = load(table_h, table)
        c_ada = load(ada_h, ada)
        c_skv = load(stale_h, skv)
        c_nz = load(noise_h, nz)
        c_emb = load(embed_h, emb)
        c_wq = load(wqkv_h, wq)
        c_ow = load(ow_h, owb.at[pl.ds(64, 576), :])
        barrier = pltpu.get_barrier_semaphore()
        greet = list(fellows.values()) + list(near.values())
        greet += [peers[n] for n in ("ap", "am", "bp", "bm", "far")]
        for peer in greet:
            pl.semaphore_signal(barrier, inc=1, device_id=peer, device_id_type=pl.DeviceIdType.MESH)
        owb[pl.ds(0, 64), :] = jnp.zeros((64, D), bf)
        owb[pl.ds(640, 64), :] = jnp.zeros((64, D), bf)
        att[...] = jnp.zeros_like(att)
        att1[...] = jnp.zeros_like(att1)
        mass1[...] = jnp.zeros_like(mass1)
        c_skv.wait()
        for b in range(3):
            kown[b] = jnp.concatenate([skv[0, b], skv[1, b]], axis=-1).reshape(64, D)
        def by_image(values, shape):
            r = lax.broadcasted_iota(jnp.int32, shape, 0)
            return jnp.where(r == 0, values[0], jnp.where(r == 1, values[1], values[2]))

        ts = [t_s[b] for b in range(3)]
        k128 = lax.broadcasted_iota(jnp.int32, (8, 128), 1).astype(f32)
        angles = by_image(ts, (8, 128)).astype(f32) * jnp.exp(-math.log(10000.0) * k128 / 128)
        feats = jnp.concatenate([jnp.cos(angles), jnp.sin(angles)], axis=1).astype(bf)
        c_tw1.wait()
        hid = jnp.dot(feats, tw1[...], preferred_element_type=f32)
        hid = (hid * jax.nn.sigmoid(hid)).astype(bf)
        c_tw2.wait()
        c_table.wait()
        NT = (((1,), (1,)), ((), ()))
        kinds = lax.broadcasted_iota(jnp.int32, (8, 1001), 1)
        picked = kinds == by_image([label_s[b] for b in range(3)], (8, 1001))
        cond = lax.dot_general(hid, tw2[...], NT, preferred_element_type=f32)
        cond = cond + lax.dot_general(
            picked.astype(f32).astype(bf), table[...], NT, preferred_element_type=f32
        )
        cond = (cond * jax.nn.sigmoid(cond)).astype(bf)
        c_ada.wait()
        for k in range(2):
            first = jnp.dot(cond, ada[:, pl.ds(k * 3 * D, 3 * D)], preferred_element_type=f32)
            part[pl.ds(4 * k, 4), pl.ds(0, 3 * D)] = first[0:4]
        for r in range(16):
            pieces[:, pl.ds(r * 128, 128)] = jnp.concatenate(
                [part[:, pl.ds(r * 256, 128)], part[:, pl.ds(r * 256 + 128, 128)]], axis=0
            ).astype(bf)
        steps = lax.broadcasted_iota(jnp.int32, (8, TSTEPS), 1)
        betas = 0.0001 + (0.02 - 0.0001) * steps.astype(f32) / (TSTEPS - 1)
        logs = jnp.where(steps <= by_image(ts, (8, TSTEPS)), jnp.log(1.0 - betas), 0.0)
        abar = jnp.exp(jnp.sum(logs, axis=1, keepdims=True))

        def wide(column):
            return jnp.stack([jnp.broadcast_to(column[b : b + 1], (4, 64)) for b in range(3)])

        keep, fuzz = wide(jnp.sqrt(abar)), wide(jnp.sqrt(1.0 - abar))

        def waves(n, start):
            place = (lax.broadcasted_iota(jnp.int32, (n, D // 4), 0) + start).astype(f32)
            k = lax.broadcasted_iota(jnp.int32, (n, D // 4), 1).astype(f32)
            args = place * jnp.exp(-math.log(10000.0) * k / (D // 4))
            return jnp.concatenate([jnp.sin(args), jnp.cos(args)], axis=1)

        rp, cp = waves(8, row * 4), waves(64, 0)
        for i in range(4):
            pos[pl.ds(i * 64, 64), :] = jnp.concatenate(
                [jnp.broadcast_to(rp[i : i + 1], (64, D // 2)), cp], axis=1
            )
        c_x.wait()
        pl.semaphore_wait(barrier, len(greet))
        for n in ("Pf", "Pd", "Pu", "Pdf", "Puf"):
            go(n)
        for c in to_all["M"]:
            c.start()
        go("R1_0")
        go("L1_0")
        for c in c_w:
            c.wait()
        for n in ("A1", "A2", "EA1", "EA2", "O", "B01", "B02", "EB01", "EB02"):
            go(n)
        for b in range(3):
            go(f"C0_{b}")
        c_nz.wait()
        c_emb.wait()
        for n in ("Pf", "Pd", "Pu", "Pdf", "Puf"):
            got(n)

        def line(d, i):
            return jnp.concatenate([xn[d, 0, :, i], xn[d, 1, :, i]], axis=-1)

        lines = [line(0, 3)] + [line(1, i) for i in range(4)] + [line(2, 0)]
        lines[0] = jnp.where(row == 0, lines[1], lines[0])
        lines[5] = jnp.where(row == 15, lines[4], lines[5])
        total = jnp.zeros((3, 4, 64), f32)
        square = jnp.zeros((3, 4, 64), f32)
        for i in range(4):
            for di in range(2):
                v = 0.75 * lines[i + 1] + 0.25 * lines[i + 2 * di]
                sides = (
                    jnp.concatenate([v[:, :, :1], v[:, :, :63]], axis=-1),
                    jnp.concatenate([v[:, :, 1:], v[:, :, 63:]], axis=-1),
                )
                for dj in range(2):
                    k = 2 * di + dj
                    n = keep * (0.75 * v + 0.25 * sides[dj]) + fuzz * nz[:, i, 4 * k : 4 * k + 4, :]
                    noisy[:, i, 4 * k : 4 * k + 4, :] = n
                    total = total + n
                    square = square + n * n
        lane1 = lax.broadcasted_iota(jnp.int32, (8, 128), 1)
        head_mid = jnp.zeros((8, 128), f32), jnp.zeros((8, 128), f32)
        for b in range(3):
            s = jnp.concatenate(
                [
                    jnp.sum(total[b], axis=1, keepdims=True),
                    jnp.sum(square[b], axis=1, keepdims=True),
                ],
                axis=0,
            )
            s = jnp.broadcast_to(s, (8, 128))
            s1 = s.astype(bf).astype(f32)
            s2 = (s - s1).astype(bf).astype(f32)
            s3 = s - s1 - s2
            head_mid = (
                jnp.where(lane1 == b, s1, jnp.where(lane1 == b + 3, s3, head_mid[0])),
                jnp.where(lane1 == b, s2, head_mid[1]),
            )
        sums = jnp.concatenate(head_mid, axis=0).astype(bf)
        both_ref[pl.ds(16, 16), :] = sums
        all15("M").wait_recv()
        at0 = pl.multiple_of(row * 256, 128)
        piece = jnp.concatenate(
            [part[:, pl.ds(at0, 128)], part[:, pl.ds(pl.multiple_of(at0 + 128, 128), 128)]], axis=0
        )
        for k in range(1, 16):
            piece = piece + rsb[k].astype(f32)
        piece = piece.astype(bf)
        both_ref[pl.ds(0, 16), :] = piece
        gs[0] = jnp.concatenate([piece, sums], axis=0)
        for c in to_all["G"]:
            c.start()
        for b in (1, 2):
            go(f"R1_{b}")
            go(f"L1_{b}")

        def norm(v):
            centre = jnp.mean(v, axis=-1, keepdims=True)
            v = v - centre
            spread = jnp.mean(v * v, axis=-1, keepdims=True)
            return v * lax.rsqrt(spread + 1e-06)

        def modrow(b, k):
            return modp[pl.ds(b + 4 * (k // 3), 1), pl.ds((k % 3) * D, D)]

        def qkv(b):
            n1 = (
                norm(tok[b].reshape(256, D).astype(f32)) * (1.0 + modrow(b, 1)) + modrow(b, 0)
            ).astype(bf)
            q = lax.dot_general(n1, wq[pl.ds(0, 576), :], NT, preferred_element_type=f32)
            qb[b, :, pl.ds(0, 576)] = (q * QS).astype(bf)
            kv = lax.dot_general(n1, wq[pl.ds(576, 1152), :], NT, preferred_element_type=f32)
            kvb[b, pl.ds(0, 256), :] = kv.astype(bf)

        lane = lax.broadcasted_iota(jnp.int32, (1, 256), 1)

        lane128 = lax.broadcasted_iota(jnp.int32, (1, 128), 1)

        def attend(b, late):
            keys = pl.ds(EARLY, NKEY - EARLY) if late else pl.ds(0, EARLY)

            def score(h):
                first = h * HD
                ks = pl.multiple_of((first // 128) * 128, 128)
                off = first - ks
                here = (lane >= off) & (lane < off + HD)
                q = qb[b, :, pl.ds(ks, 256)]
                q = jnp.where(here, q, jnp.zeros_like(q))
                return lax.dot_general(
                    q, kvb[b, keys, pl.ds(ks, 256)], NT, preferred_element_type=f32
                )

            def mix(h, s):
                first = h * HD
                vs = pl.multiple_of(jnp.minimum(((576 + first) // 128) * 128, 896), 128)
                voff = 576 + first - vs
                mine = (lane >= voff) & (lane < voff + HD)
                cols = pl.ds(pl.multiple_of(vs - 512, 128), 256)
                chosen = lane128 == h
                if late:
                    top = jnp.max(s, axis=1, keepdims=True) + 2.0
                    before = jnp.sum(jnp.where(chosen, mass1[b], 0.0), axis=1, keepdims=True)
                    top = jnp.maximum(top, before)
                    p = jnp.exp2(s - (top - 2.0))
                    kept = jnp.exp2(before - top)
                    mass = jnp.sum(p, axis=1, keepdims=True) + kept
                    o = jnp.dot(p.astype(bf), kvb[b, keys, pl.ds(vs, 256)], preferred_element_type=f32)
                    o = (o + kept * att1[b, :, cols]) * (1.0 / mass)
                    o = o.astype(bf).reshape(4, 2, 32, 256)
                    att[b, :, :, :, cols] = jnp.where(
                        mine.reshape(1, 1, 1, 256), o, att[b, :, :, :, cols]
                    )
                    return
                fresh, old = s[:, :256], s[:, 256:]
                top = jnp.maximum(
                    jnp.max(fresh, axis=1, keepdims=True), jnp.max(old, axis=1, keepdims=True) + 2.0
                )
                p0 = jnp.exp2(fresh - top)
                p1 = jnp.exp2(old - (top - 2.0))
                mass = jnp.sum(p0, axis=1, keepdims=True) + jnp.sum(p1, axis=1, keepdims=True)
                o = jnp.dot(
                    p0.astype(bf), kvb[b, pl.ds(0, 256), pl.ds(vs, 256)],
                    preferred_element_type=f32,
                ) + jnp.dot(
                    p1.astype(bf), kvb[b, pl.ds(256, EARLY - 256), pl.ds(vs, 256)],
                    preferred_element_type=f32,
                )
                att1[b, :, cols] = jnp.where(mine, o * (1.0 / mass), att1[b, :, cols])
                mass1[b] = jnp.where(chosen, top + jnp.log2(mass), mass1[b])

            def some(i, _):
                hs = [i * UNROLL + j for j in range(UNROLL)]
                ss = [score(h) for h in hs]
                for h, s in zip(hs, ss):
                    mix(h, s)
                return 0

            lax.fori_loop(0, 8 // UNROLL, some, 0)

        def project(b):
            rows = pl.ds(b * 128, 128)
            p = acc[rows, :] + jnp.dot(attr[b].reshape(128, 640), owb[pl.ds(640, 640), :], preferred_element_type=f32)
            t = tok[b, :, head].reshape(128, D).astype(f32)
            m = (t + modrow(b, 2) * p).astype(bf)
            mid[pl.ds(b * 128, 128), :] = m
            n = norm(m.astype(f32)) * (1.0 + modrow(b, 4)) + modrow(b, 3)
            n2[pl.ds(b * 128, 128), :] = n.astype(bf)
            acc[rows, :] = jnp.zeros((128, D), f32)

        def project_own(b):
            mine = att[b, :, head].reshape(128, 640)
            acc[pl.ds(b * 128, 128), :] = jnp.dot(
                mine, owb[pl.ds(0, 640), :], preferred_element_type=f32
            )

        def feed(first, count):
            rows = [pl.ds(first + i * 768, 768) for i in range(count)]
            hids = [
                lax.dot_general(n2[...], wb[0, r, :], NT, preferred_element_type=f32) for r in rows
            ]
            for r, hid in zip(rows, hids):
                hid = jax.nn.gelu(hid, approximate=True).astype(bf)
                acc[...] += jnp.dot(hid, wb[1, r, :], preferred_element_type=f32)

        def kstep(d, b):
            got(f"R{d}_{b}")
            got(f"L{d}_{b}")
            if d < 4:
                go(f"R{d + 1}_{b}")
                go(f"L{d + 1}_{b}")

        def fwd(tag):
            got(tag + "1")
            go(tag + "3a")
            got(tag + "2")
            go(tag + "3b")

        def done(tag):
            got(tag + "3a")
            got(tag + "3b")

        kstep(1, 0)
        all15("G").wait_recv()
        first, second = jnp.zeros((8, 128), f32), jnp.zeros((8, 128), f32)
        for k in range(16):
            g = gs[k].astype(f32)
            first, second = first + g[16:24], second + g[24:32]
            lo = pl.multiple_of(((row + 16 - k) % 16) * 256, 128)
            modp[:, pl.ds(lo, 128)] = g[0:8]
            modp[:, pl.ds(pl.multiple_of(lo + 128, 128), 128)] = g[8:16]
        shares, gains = [], []
        for b in range(3):
            chosen = jnp.where((lane1 == b) | (lane1 == b + 3), first, 0.0)
            chosen = chosen + jnp.where(lane1 == b, second, 0.0)
            col_b = jnp.sum(chosen, axis=1, keepdims=True) / 16384.0
            centre = col_b[0:4]
            gain = lax.rsqrt(col_b[4:8] - centre * centre + 1e-05)
            shares.append(jnp.concatenate([centre] * 4, axis=0))
            gains.append(jnp.concatenate([gain] * 4, axis=0))
        whi = emb[...].astype(bf)
        wlo = (emb[...] - whi.astype(f32)).astype(bf)
        w3 = jnp.concatenate([whi, whi, wlo], axis=0)
        c_wq.wait()
        for b in range(3):
            for i in range(4):
                n = (noisy[b, i] - shares[b]) * gains[b]
                hi = n.astype(bf)
                lo = (n - hi.astype(f32)).astype(bf)
                e = lax.dot_general(
                    jnp.concatenate([hi, lo, hi], axis=0), w3, (((0,), (0,)), ((), ())),
                    preferred_element_type=f32,
                )
                e = (e + pos[pl.ds(i * 64, 64), :]).astype(bf)
                tok[b, i] = e.reshape(2, 32, D)
        def both_kinds(act, tag):
            act(tag)
            act("E" + tag)

        def begin(tag):
            go(tag + "1")
            go(tag + "2")

        kstep(1, 1)
        qkv(0)
        kstep(1, 2)
        both_kinds(fwd, "A")
        for g in (1, 2):
            both_kinds(begin, f"B{g}")
        qkv(1)
        kstep(2, 0)
        go("C1_0")
        qkv(2)
        kstep(2, 1)
        go("C1_1")
        got("C0_0")
        got("C1_0")
        attend(0, False)
        kstep(2, 2)
        go("C1_2")
        both_kinds(fwd, "B0")
        both_kinds(done, "A")
        both_kinds(begin, "B3")
        got("C0_1")
        got("C1_1")
        kstep(3, 0)
        attend(1, False)
        kstep(3, 1)
        go("S0a")
        got("C0_2")
        got("C1_2")
        attend(2, False)
        kstep(3, 2)
        kstep(4, 0)
        go("C2_0")
        kstep(4, 1)
        go("C2_1")
        got("O")
        go("OZ")
        go("OS0")
        got("C2_0")
        attend(0, True)
        go("X0")
        kstep(4, 2)
        go("C2_2")
        both_kinds(fwd, "B1")
        got("C2_1")
        attend(1, True)
        go("X1")
        both_kinds(done, "B0")
        go("S0b")
        go("S1a")
        got("C2_2")
        attend(2, True)
        go("X2")
        both_kinds(fwd, "B2")
        go("S2a")
        c_ow.wait()
        project_own(0)
        project_own(1)
        got("OZ")
        go("OS1")
        project_own(2)
        got("OS0")
        got("X0")
        got("OS1")
        project(0)
        got("X1")
        project(1)
        both_kinds(fwd, "B3")
        go("S3a")
        got("X2")
        project(2)
        got("S0a")
        got("S1a")
        feed(0, 2)
        both_kinds(done, "B1")
        go("S1b")
        both_kinds(done, "B2")
        go("S2b")
        got("S2a")
        got("S3a")
        feed(1536, 2)
        both_kinds(done, "B3")
        go("S3b")
        got("S0b")
        got("S1b")
        feed(3072, 1)
        got("S2b")
        got("S3b")
        feed(3840, 1)

        def finish():
            for b in range(3):
                r = pl.ds(b * 128, 128)
                outb[r, :] = (mid[r, :].astype(f32) + modrow(b, 5) * acc[r, :]).astype(bf)
            for b in range(3):
                r = pl.ds(b * 128, 128)
                load(outb.at[r, :], out_ref.at[r, :])
            for c in loads[-3:]:
                c.wait()

        finish()
        for c in copies.values():
            c.wait_send()
        all15("M").wait_send()
        all15("G").wait_send()

    any_spec = pl.BlockSpec(memory_space=pl.ANY)
    n_copies = 2 * 20 + 8 + 3 * 12 + 4 + 5 + 2
    return pl.pallas_call(
        kernel,
        out_shape=jax.ShapeDtypeStruct((384, D), bf),
        in_specs=[pl.BlockSpec(memory_space=pltpu.SMEM)] * 2 + [any_spec] * 12,
        out_specs=any_spec,
        scratch_shapes=[
            pltpu.VMEM((3, 2, 3, 4, 4, 32), f32),
            pltpu.VMEM((3, 4, 16, 64), f32),
            pltpu.VMEM((16, D), f32),
            pltpu.VMEM((256, D), f32),
            pltpu.VMEM((256, D), bf),
            pltpu.VMEM((72, D), bf),
            pltpu.VMEM((72, 1001), bf),
            pltpu.VMEM((72, 6 * D), bf),
            pltpu.VMEM((2, 3, 2, 32, 576), bf),
            pltpu.VMEM((3, 64, D), bf),
            pltpu.VMEM((3, 256, 640), f32),
            pltpu.VMEM((3, 256, 128), f32),
            pltpu.VMEM((8, 4096), f32),
            pltpu.VMEM((16, 2048), bf),
            pltpu.VMEM((16, 16, 128), bf),
            pltpu.VMEM((32, 128), bf),
            pltpu.VMEM((16, 32, 128), bf),
            pltpu.VMEM((8, 4096), f32),
            pltpu.VMEM((3, 4, 16, 64), f32),
            pltpu.VMEM((3, 4, 2, 32, D), bf),
            pltpu.VMEM((1728, D), bf),
            pltpu.VMEM((3, NKEY, D), bf),
            pltpu.VMEM((2, HID, D), bf),
            pltpu.VMEM((1280, D), bf),
            pltpu.VMEM((3, 256, 640), bf),
            pltpu.VMEM((3, 4, 2, 32, 640), bf),
            pltpu.VMEM((3, 4, 32, 640), bf),
            pltpu.VMEM((384, D), bf),
            pltpu.VMEM((384, D), bf),
            pltpu.VMEM((384, D), f32),
            pltpu.VMEM((384, D), bf),
            pltpu.SemaphoreType.DMA((n_copies,)),
            pltpu.SemaphoreType.DMA((n_copies,)),
            pltpu.SemaphoreType.DMA((18,)),
        ],
        compiler_params=pltpu.CompilerParams(
            collective_id=0, has_side_effects=True, vmem_limit_bytes=58_000_000
        ),
    )(t_index, labels, x_lo, noise, embed, tw1, tw2, table, ada, stale, wqkv, ow, fc1, fc2)


def body(
    x_lo,
    noise,
    t_index,
    labels,
    stale_kv,
    embed_w,
    t_w1,
    t_w2,
    class_table,
    ada_w,
    qkv_w,
    out_w,
    fc1_w,
    fc2_w,
):
    head_count = lax.axis_size("head")
    tile_rows, full_cols = noise.shape[1], noise.shape[2]
    batch, width = noise.shape[0], embed_w.shape[1]
    half = full_cols // head_count
    local_width = qkv_w.shape[2]
    out = fused_block(
        t_index,
        labels,
        x_lo.transpose(0, 1, 3, 2),
        noise.transpose(0, 1, 3, 2),
        embed_w,
        t_w1,
        t_w2.T,
        class_table.T,
        ada_w,
        stale_kv,
        qkv_w.transpose(1, 2, 0).reshape(3 * local_width, width),
        out_w,
        fc1_w.T,
        fc2_w.T,
    )
    return out.reshape(batch, tile_rows, half, width)


def solution(mesh):
    placed = (
        P("col", "row", "head", None),
        P("col", "row", None, None),
        P("col"),
        P("col"),
        P(None, "col", "row", None, "head"),
        P(),
        P(),
        P(None, "row"),
        P(None, "row"),
        P("row", None),
        P(None, None, "head"),
        P("head", None),
        P(None, ("col", "head")),
        P(None, ("col", "head")),
    )
    return jax.shard_map(
        body, mesh=mesh, in_specs=placed, out_specs=P("col", "row", "head", None), check_vma=False
    )
```

```python
import math

import jax
import jax.numpy as jnp
from jax import lax
from jax.experimental import pallas as pl
from jax.experimental.pallas import tpu as pltpu
from jax.sharding import PartitionSpec as P

HD = 72
TSTEPS = 1000


def fused_block(t_index, labels, x_lo, noise, embed, tw1, tw2, table, ada, stale, wqkv, ow, fc1, fc2):
    D = 1152
    L2E = 1.4426950408889634
    QS = L2E / math.sqrt(HD)
    bf, f32 = jnp.bfloat16, jnp.float32
    NKEY = 256 + 15 * 64
    HID = 4608
    UNROLL = 2
    EARLY = 256 + 9 * 64

    def kernel(
        t_s, label_s, x_h, noise_h, embed_h, tw1_h, tw2_h, table_h, ada_h, stale_h, wqkv_h, ow_h, fc1_h,
        fc2_h, out_ref, xn, nz, emb, pos, tw1, tw2, table, ada, skv, kown, att1, mass1, part, pieces, rsb, both_ref, gs, modp, noisy,
        tok, wq, kvb, wb, owb, qb, att, attr, n2, mid, acc, outb, send, recv, local,
    ):
        row, col, head = lax.axis_index("row"), lax.axis_index("col"), lax.axis_index("head")
        z, core = row // 2, row % 2
        x, y = head * 2 + col // 4, col % 4

        def at(x_, y_, z_, core_):
            return (z_ * 2 + core_, (x_ % 2) * 4 + y_, x_ // 2)

        peers = {
            "sib": at(x, y, z, 1 - core),
            "zp": at(x, y, (z + 1) % 8, core),
            "zm": at(x, y, (z + 7) % 8, core),
            "ap": at((x + core) % 4, (y + 1 - core) % 4, z, core),
            "am": at((x + 4 - core) % 4, (y + 3 + core) % 4, z, core),
            "bp": at((x + 1 - core) % 4, (y + core) % 4, z, core),
            "bm": at((x + 3 + core) % 4, (y + 4 - core) % 4, z, core),
            "far": at((x + 2) % 4, y, z, core),
        }
        other = at(3 - x, y, z, core)
        twin = at(x, y, z + 1 - 2 * (z % 2), core)
        near = {}
        for dr in (1, 15):
            near[f"h{dr}"] = ((row + dr) % 16, col, 1 - head)
        fellows = {k: ((row + k) % 16, col, head) for k in range(1, 16)}

        copies = {}
        order = {"n": 0}

        def remote(name, src, dst, peer):
            k = order["n"]
            order["n"] = k + 1
            c = pltpu.make_async_remote_copy(
                src_ref=src, dst_ref=dst, send_sem=send.at[k], recv_sem=recv.at[k],
                device_id=peer, device_id_type=pl.DeviceIdType.MESH,
            )
            copies[name] = c
            return c

        def go(name):
            copies[name].start()

        def got(name):
            copies[name].wait_recv()

        loads = []

        def load(src, dst):
            c = pltpu.make_async_copy(src, dst, local.at[len(loads)])
            loads.append(c)
            c.start()
            return c

        SIZE, PLUS = {"": 112, "E": 32}, {"": 64, "E": 16}

        def blk(kind, group, j, part=None):
            lo, n = {
                None: (0, SIZE[kind]), 0: (0, PLUS[kind]), 1: (PLUS[kind], SIZE[kind] - PLUS[kind])
            }[part]
            if j < 3:
                base = group * 864 + (336 if kind else 0) + j * SIZE[kind]
            else:
                base = 3456 + group * 288 + (112 if kind else 0)
            return wb.at[:, pl.ds(base + lo, n), :]

        def ring(tag, sides, place):
            p, m = sides
            remote(tag + "1", place(0, None), place(1, None), p)
            remote(tag + "2", place(0, None), place(2, None), m)
            remote(tag + "3a", place(1, 0), place(3, 0), p)
            remote(tag + "3b", place(2, 1), place(3, 1), m)

        along = {
            "A": (peers["ap"], peers["am"]),
            "B": (peers["bp"], peers["bm"]),
            "EA": (at((x + 1) % 4, y, z, core), at((x + 3) % 4, y, z, core)),
            "EB": (at(x, (y + 1) % 4, z, core), at(x, (y + 3) % 4, z, core)),
        }
        for kind in ("", "E"):
            ring(kind + "A", along[kind + "A"], lambda g, part, kind=kind: blk(kind, g, 0, part))
            for g in range(4):
                ring(
                    f"{kind}B{g}", along[kind + "B"],
                    lambda j, part, g=g, kind=kind: blk(kind, g, j, part),
                )
        for g in range(4):
            for name, lo, n in ((f"S{g}a", g * 864, 432), (f"S{g}b", 3456 + g * 288, 144)):
                remote(
                    name, wb.at[:, pl.ds(lo, n), :], wb.at[:, pl.ds(lo + n, n), :], peers["sib"]
                )

        def slot(b, s, lo=0, n=64):
            return kvb.at[b, pl.ds(256 + s * 64 + lo, n), :]

        for b in range(3):
            own = kown.at[b]
            zp, zm = peers["zp"], peers["zm"]
            right, left = (0, 2, 9), (1, 3, 10)
            remote(f"R1_{b}", own, slot(b, 0), zp)
            remote(f"L1_{b}", own, slot(b, 1), zm)
            for d in (1, 2):
                remote(f"R{d + 1}_{b}", slot(b, right[d - 1]), slot(b, right[d]), zp)
                remote(f"L{d + 1}_{b}", slot(b, left[d - 1]), slot(b, left[d]), zm)
            remote(f"R4_{b}", slot(b, 9, 0, 32), slot(b, 11, 0, 32), zp)
            remote(f"L4_{b}", slot(b, 10, 32, 32), slot(b, 11, 32, 32), zm)
            remote(f"C0_{b}", own, slot(b, 4), peers["sib"])
            remote(f"C1_{b}", slot(b, 0, 0, 256), slot(b, 5, 0, 256), peers["sib"])
            remote(f"C2_{b}", slot(b, 9, 0, 192), slot(b, 12, 0, 192), peers["sib"])
            remote(
                f"X{b}", att.at[b, :, 1 - head], attr.at[b], peers["far"],
            )
        part_at = lambda p: p * 288 + core * 144
        ow_own = pl.ds(pl.multiple_of(part_at(z % 2), 16), 144)
        far0 = pl.ds(pl.multiple_of(704 + part_at(z % 2), 16), 144)
        far1 = pl.ds(pl.multiple_of(704 + part_at(1 - z % 2), 16), 144)
        remote("O", ow_h.at[ow_own, :], owb.at[far0, :], other)
        remote("OZ", owb.at[far0, :], owb.at[far0, :], twin)
        remote("OS0", owb.at[far0, :], owb.at[far0, :], peers["sib"])
        remote("OS1", owb.at[far1, :], owb.at[far1, :], peers["sib"])
        remote("Pf", xn.at[1, head], xn.at[1, head], peers["far"])
        remote("Pd", xn.at[1, head], xn.at[0, head], fellows[1])
        remote("Pu", xn.at[1, head], xn.at[2, head], fellows[15])
        remote("Pdf", xn.at[1, head], xn.at[0, head], near["h1"])
        remote("Puf", xn.at[1, head], xn.at[2, head], near["h15"])
        shared = {}
        for tag in "MG":
            shared[tag] = order["n"]
            order["n"] += 1
        to_all = {"M": [], "G": []}
        for k in range(1, 16):
            to = (row + k) % 16
            chunk = pl.ds(pl.multiple_of(to * 128, 128), 128)
            for tag, src, dst in (
                ("M", pieces.at[:, chunk], rsb.at[k]), ("G", both_ref, gs.at[k])
            ):
                to_all[tag].append(
                    pltpu.make_async_remote_copy(
                        src_ref=src, dst_ref=dst, send_sem=send.at[shared[tag]],
                        recv_sem=recv.at[shared[tag]], device_id=fellows[k],
                        device_id_type=pl.DeviceIdType.MESH,
                    )
                )

        def all15(tag):
            buf = {"M": rsb, "G": gs}[tag].at[pl.ds(1, 15)]
            return pltpu.make_async_remote_copy(
                src_ref=buf, dst_ref=buf, send_sem=send.at[shared[tag]],
                recv_sem=recv.at[shared[tag]], device_id=fellows[1],
                device_id_type=pl.DeviceIdType.MESH,
            )

        c_w = []
        for kind, lo in (("", 0), ("E", 112)):
            rows = pl.ds(pl.multiple_of(core * 144 + lo, 16), SIZE[kind])
            for k, w_h in enumerate((fc1_h, fc2_h)):
                c_w.append(load(w_h.at[rows, :], wb.at[k, pl.ds(336 if kind else 0, SIZE[kind]), :]))
        c_x = load(x_h, xn.at[1, head])
        c_tw1 = load(tw1_h, tw1)
        c_tw2 = load(tw2_h, tw2)
        c_table = load(table_h, table)
        c_ada = load(ada_h, ada)
        c_skv = load(stale_h, skv)
        c_nz = load(noise_h, nz)
        c_emb = load(embed_h, emb)
        c_wq = load(wqkv_h, wq)
        c_ow = load(ow_h, owb.at[pl.ds(64, 576), :])
        barrier = pltpu.get_barrier_semaphore()
        greet = list(fellows.values()) + list(near.values())
        greet += [peers[n] for n in ("ap", "am", "bp", "bm", "far")]
        for peer in greet:
            pl.semaphore_signal(barrier, inc=1, device_id=peer, device_id_type=pl.DeviceIdType.MESH)
        owb[pl.ds(0, 64), :] = jnp.zeros((64, D), bf)
        owb[pl.ds(640, 64), :] = jnp.zeros((64, D), bf)
        att[...] = jnp.zeros_like(att)
        att1[...] = jnp.zeros_like(att1)
        mass1[...] = jnp.zeros_like(mass1)
        c_skv.wait()
        for b in range(3):
            kown[b] = jnp.concatenate([skv[0, b], skv[1, b]], axis=-1).reshape(64, D)
        def by_image(values, shape):
            r = lax.broadcasted_iota(jnp.int32, shape, 0)
            return jnp.where(r == 0, values[0], jnp.where(r == 1, values[1], values[2]))

        ts = [t_s[b] for b in range(3)]
        k128 = lax.broadcasted_iota(jnp.int32, (8, 128), 1).astype(f32)
        angles = by_image(ts, (8, 128)).astype(f32) * jnp.exp(-math.log(10000.0) * k128 / 128)
        feats = jnp.concatenate([jnp.cos(angles), jnp.sin(angles)], axis=1).astype(bf)
        c_tw1.wait()
        hid = jnp.dot(feats, tw1[...], preferred_element_type=f32)
        hid = (hid * jax.nn.sigmoid(hid)).astype(bf)
        c_tw2.wait()
        c_table.wait()
        NT = (((1,), (1,)), ((), ()))
        kinds = lax.broadcasted_iota(jnp.int32, (8, 1001), 1)
        picked = kinds == by_image([label_s[b] for b in range(3)], (8, 1001))
        cond = lax.dot_general(hid, tw2[...], NT, preferred_element_type=f32)
        cond = cond + lax.dot_general(
            picked.astype(f32).astype(bf), table[...], NT, preferred_element_type=f32
        )
        cond = (cond * jax.nn.sigmoid(cond)).astype(bf)
        c_ada.wait()
        for k in range(2):
            first = jnp.dot(cond, ada[:, pl.ds(k * 3 * D, 3 * D)], preferred_element_type=f32)
            part[pl.ds(4 * k, 4), pl.ds(0, 3 * D)] = first[0:4]
        for r in range(16):
            pieces[:, pl.ds(r * 128, 128)] = jnp.concatenate(
                [part[:, pl.ds(r * 256, 128)], part[:, pl.ds(r * 256 + 128, 128)]], axis=0
            ).astype(bf)
        steps = lax.broadcasted_iota(jnp.int32, (8, TSTEPS), 1)
        betas = 0.0001 + (0.02 - 0.0001) * steps.astype(f32) / (TSTEPS - 1)
        logs = jnp.where(steps <= by_image(ts, (8, TSTEPS)), jnp.log(1.0 - betas), 0.0)
        abar = jnp.exp(jnp.sum(logs, axis=1, keepdims=True))

        def wide(column):
            return jnp.stack([jnp.broadcast_to(column[b : b + 1], (4, 64)) for b in range(3)])

        keep, fuzz = wide(jnp.sqrt(abar)), wide(jnp.sqrt(1.0 - abar))

        def waves(n, start):
            place = (lax.broadcasted_iota(jnp.int32, (n, D // 4), 0) + start).astype(f32)
            k = lax.broadcasted_iota(jnp.int32, (n, D // 4), 1).astype(f32)
            args = place * jnp.exp(-math.log(10000.0) * k / (D // 4))
            return jnp.concatenate([jnp.sin(args), jnp.cos(args)], axis=1)

        rp, cp = waves(8, row * 4), waves(64, 0)
        for i in range(4):
            pos[pl.ds(i * 64, 64), :] = jnp.concatenate(
                [jnp.broadcast_to(rp[i : i + 1], (64, D // 2)), cp], axis=1
            )
        c_x.wait()
        pl.semaphore_wait(barrier, len(greet))
        for n in ("Pf", "Pd", "Pu", "Pdf", "Puf"):
            go(n)
        for c in to_all["M"]:
            c.start()
        go("R1_0")
        go("L1_0")
        for c in c_w:
            c.wait()
        for n in ("A1", "A2", "EA1", "EA2", "O", "B01", "B02", "EB01", "EB02"):
            go(n)
        for b in range(3):
            go(f"C0_{b}")
        c_nz.wait()
        c_emb.wait()
        for n in ("Pf", "Pd", "Pu", "Pdf", "Puf"):
            got(n)

        def line(d, i):
            return jnp.concatenate([xn[d, 0, :, i], xn[d, 1, :, i]], axis=-1)

        lines = [line(0, 3)] + [line(1, i) for i in range(4)] + [line(2, 0)]
        lines[0] = jnp.where(row == 0, lines[1], lines[0])
        lines[5] = jnp.where(row == 15, lines[4], lines[5])
        total = jnp.zeros((3, 4, 64), f32)
        square = jnp.zeros((3, 4, 64), f32)
        for i in range(4):
            for di in range(2):
                v = 0.75 * lines[i + 1] + 0.25 * lines[i + 2 * di]
                sides = (
                    jnp.concatenate([v[:, :, :1], v[:, :, :63]], axis=-1),
                    jnp.concatenate([v[:, :, 1:], v[:, :, 63:]], axis=-1),
                )
                for dj in range(2):
                    k = 2 * di + dj
                    n = keep * (0.75 * v + 0.25 * sides[dj]) + fuzz * nz[:, i, 4 * k : 4 * k + 4, :]
                    noisy[:, i, 4 * k : 4 * k + 4, :] = n
                    total = total + n
                    square = square + n * n
        lane1 = lax.broadcasted_iota(jnp.int32, (8, 128), 1)
        head_mid = jnp.zeros((8, 128), f32), jnp.zeros((8, 128), f32)
        for b in range(3):
            s = jnp.concatenate(
                [
                    jnp.sum(total[b], axis=1, keepdims=True),
                    jnp.sum(square[b], axis=1, keepdims=True),
                ],
                axis=0,
            )
            s = jnp.broadcast_to(s, (8, 128))
            s1 = s.astype(bf).astype(f32)
            s2 = (s - s1).astype(bf).astype(f32)
            s3 = s - s1 - s2
            head_mid = (
                jnp.where(lane1 == b, s1, jnp.where(lane1 == b + 3, s3, head_mid[0])),
                jnp.where(lane1 == b, s2, head_mid[1]),
            )
        sums = jnp.concatenate(head_mid, axis=0).astype(bf)
        both_ref[pl.ds(16, 16), :] = sums
        all15("M").wait_recv()
        at0 = pl.multiple_of(row * 256, 128)
        piece = jnp.concatenate(
            [part[:, pl.ds(at0, 128)], part[:, pl.ds(pl.multiple_of(at0 + 128, 128), 128)]], axis=0
        )
        for k in range(1, 16):
            piece = piece + rsb[k].astype(f32)
        piece = piece.astype(bf)
        both_ref[pl.ds(0, 16), :] = piece
        gs[0] = jnp.concatenate([piece, sums], axis=0)
        for c in to_all["G"]:
            c.start()
        for b in (1, 2):
            go(f"R1_{b}")
            go(f"L1_{b}")

        def norm(v):
            centre = jnp.mean(v, axis=-1, keepdims=True)
            v = v - centre
            spread = jnp.mean(v * v, axis=-1, keepdims=True)
            return v * lax.rsqrt(spread + 1e-06)

        def modrow(b, k):
            return modp[pl.ds(b + 4 * (k // 3), 1), pl.ds((k % 3) * D, D)]

        def qkv(b):
            n1 = (
                norm(tok[b].reshape(256, D).astype(f32)) * (1.0 + modrow(b, 1)) + modrow(b, 0)
            ).astype(bf)
            q = lax.dot_general(n1, wq[pl.ds(0, 576), :], NT, preferred_element_type=f32)
            qb[b, :, pl.ds(0, 576)] = (q * QS).astype(bf)
            kv = lax.dot_general(n1, wq[pl.ds(576, 1152), :], NT, preferred_element_type=f32)
            kvb[b, pl.ds(0, 256), :] = kv.astype(bf)

        lane = lax.broadcasted_iota(jnp.int32, (1, 256), 1)

        lane128 = lax.broadcasted_iota(jnp.int32, (1, 128), 1)

        def attend(b, late):
            keys = pl.ds(EARLY, NKEY - EARLY) if late else pl.ds(0, EARLY)

            def score(h):
                first = h * HD
                ks = pl.multiple_of((first // 128) * 128, 128)
                off = first - ks
                here = (lane >= off) & (lane < off + HD)
                q = qb[b, :, pl.ds(ks, 256)]
                q = jnp.where(here, q, jnp.zeros_like(q))
                return lax.dot_general(
                    q, kvb[b, keys, pl.ds(ks, 256)], NT, preferred_element_type=f32
                )

            def mix(h, s):
                first = h * HD
                vs = pl.multiple_of(jnp.minimum(((576 + first) // 128) * 128, 896), 128)
                voff = 576 + first - vs
                mine = (lane >= voff) & (lane < voff + HD)
                cols = pl.ds(pl.multiple_of(vs - 512, 128), 256)
                chosen = lane128 == h
                if late:
                    top = jnp.max(s, axis=1, keepdims=True) + 2.0
                    before = jnp.sum(jnp.where(chosen, mass1[b], 0.0), axis=1, keepdims=True)
                    top = jnp.maximum(top, before)
                    p = jnp.exp2(s - (top - 2.0))
                    kept = jnp.exp2(before - top)
                    mass = jnp.sum(p, axis=1, keepdims=True) + kept
                    o = jnp.dot(p.astype(bf), kvb[b, keys, pl.ds(vs, 256)], preferred_element_type=f32)
                    o = (o + kept * att1[b, :, cols]) * (1.0 / mass)
                    o = o.astype(bf).reshape(4, 2, 32, 256)
                    att[b, :, :, :, cols] = jnp.where(
                        mine.reshape(1, 1, 1, 256), o, att[b, :, :, :, cols]
                    )
                    return
                fresh, old = s[:, :256], s[:, 256:]
                top = jnp.maximum(
                    jnp.max(fresh, axis=1, keepdims=True), jnp.max(old, axis=1, keepdims=True) + 2.0
                )
                p0 = jnp.exp2(fresh - top)
                p1 = jnp.exp2(old - (top - 2.0))
                mass = jnp.sum(p0, axis=1, keepdims=True) + jnp.sum(p1, axis=1, keepdims=True)
                o = jnp.dot(
                    p0.astype(bf), kvb[b, pl.ds(0, 256), pl.ds(vs, 256)],
                    preferred_element_type=f32,
                ) + jnp.dot(
                    p1.astype(bf), kvb[b, pl.ds(256, EARLY - 256), pl.ds(vs, 256)],
                    preferred_element_type=f32,
                )
                att1[b, :, cols] = jnp.where(mine, o * (1.0 / mass), att1[b, :, cols])
                mass1[b] = jnp.where(chosen, top + jnp.log2(mass), mass1[b])

            def some(i, _):
                hs = [i * UNROLL + j for j in range(UNROLL)]
                ss = [score(h) for h in hs]
                for h, s in zip(hs, ss):
                    mix(h, s)
                return 0

            lax.fori_loop(0, 8 // UNROLL, some, 0)

        def project(b):
            rows = pl.ds(b * 128, 128)
            p = acc[rows, :] + jnp.dot(attr[b].reshape(128, 640), owb[pl.ds(640, 640), :], preferred_element_type=f32)
            t = tok[b, :, head].reshape(128, D).astype(f32)
            m = (t + modrow(b, 2) * p).astype(bf)
            mid[pl.ds(b * 128, 128), :] = m
            n = norm(m.astype(f32)) * (1.0 + modrow(b, 4)) + modrow(b, 3)
            n2[pl.ds(b * 128, 128), :] = n.astype(bf)
            acc[rows, :] = jnp.zeros((128, D), f32)

        def project_own(b):
            mine = att[b, :, head].reshape(128, 640)
            acc[pl.ds(b * 128, 128), :] = jnp.dot(
                mine, owb[pl.ds(0, 640), :], preferred_element_type=f32
            )

        def feed(first, count):
            rows = [pl.ds(first + i * 768, 768) for i in range(count)]
            hids = [
                lax.dot_general(n2[...], wb[0, r, :], NT, preferred_element_type=f32) for r in rows
            ]
            for r, hid in zip(rows, hids):
                hid = jax.nn.gelu(hid, approximate=True).astype(bf)
                acc[...] += jnp.dot(hid, wb[1, r, :], preferred_element_type=f32)

        def kstep(d, b):
            got(f"R{d}_{b}")
            got(f"L{d}_{b}")
            if d < 4:
                go(f"R{d + 1}_{b}")
                go(f"L{d + 1}_{b}")

        def fwd(tag):
            got(tag + "1")
            go(tag + "3a")
            got(tag + "2")
            go(tag + "3b")

        def done(tag):
            got(tag + "3a")
            got(tag + "3b")

        kstep(1, 0)
        all15("G").wait_recv()
        first, second = jnp.zeros((8, 128), f32), jnp.zeros((8, 128), f32)
        for k in range(16):
            g = gs[k].astype(f32)
            first, second = first + g[16:24], second + g[24:32]
            lo = pl.multiple_of(((row + 16 - k) % 16) * 256, 128)
            modp[:, pl.ds(lo, 128)] = g[0:8]
            modp[:, pl.ds(pl.multiple_of(lo + 128, 128), 128)] = g[8:16]
        shares, gains = [], []
        for b in range(3):
            chosen = jnp.where((lane1 == b) | (lane1 == b + 3), first, 0.0)
            chosen = chosen + jnp.where(lane1 == b, second, 0.0)
            col_b = jnp.sum(chosen, axis=1, keepdims=True) / 16384.0
            centre = col_b[0:4]
            gain = lax.rsqrt(col_b[4:8] - centre * centre + 1e-05)
            shares.append(jnp.concatenate([centre] * 4, axis=0))
            gains.append(jnp.concatenate([gain] * 4, axis=0))
        whi = emb[...].astype(bf)
        wlo = (emb[...] - whi.astype(f32)).astype(bf)
        w3 = jnp.concatenate([whi, whi, wlo], axis=0)
        c_wq.wait()
        for b in range(3):
            for i in range(4):
                n = (noisy[b, i] - shares[b]) * gains[b]
                hi = n.astype(bf)
                lo = (n - hi.astype(f32)).astype(bf)
                e = lax.dot_general(
                    jnp.concatenate([hi, lo, hi], axis=0), w3, (((0,), (0,)), ((), ())),
                    preferred_element_type=f32,
                )
                e = (e + pos[pl.ds(i * 64, 64), :]).astype(bf)
                tok[b, i] = e.reshape(2, 32, D)
        def both_kinds(act, tag):
            act(tag)
            act("E" + tag)

        def begin(tag):
            go(tag + "1")
            go(tag + "2")

        kstep(1, 1)
        qkv(0)
        kstep(1, 2)
        both_kinds(fwd, "A")
        for g in (1, 2):
            both_kinds(begin, f"B{g}")
        qkv(1)
        kstep(2, 0)
        go("C1_0")
        qkv(2)
        kstep(2, 1)
        go("C1_1")
        got("C0_0")
        got("C1_0")
        attend(0, False)
        kstep(2, 2)
        go("C1_2")
        both_kinds(fwd, "B0")
        got("C0_1")
        got("C1_1")
        kstep(3, 0)
        attend(1, False)
        both_kinds(done, "A")
        both_kinds(begin, "B3")
        kstep(3, 1)
        go("S0a")
        got("C0_2")
        got("C1_2")
        attend(2, False)
        kstep(3, 2)
        kstep(4, 0)
        go("C2_0")
        kstep(4, 1)
        go("C2_1")
        got("O")
        go("OZ")
        go("OS0")
        got("C2_0")
        attend(0, True)
        go("X0")
        kstep(4, 2)
        go("C2_2")
        both_kinds(fwd, "B1")
        got("C2_1")
        attend(1, True)
        go("X1")
        both_kinds(done, "B0")
        go("S0b")
        go("S1a")
        got("C2_2")
        attend(2, True)
        go("X2")
        both_kinds(fwd, "B2")
        c_ow.wait()
        project_own(0)
        got("OZ")
        go("OS1")
        go("S2a")
        project_own(1)
        project_own(2)
        got("OS0")
        got("X0")
        got("OS1")
        project(0)
        got("X1")
        project(1)
        both_kinds(fwd, "B3")
        go("S3a")
        got("X2")
        project(2)
        got("S0a")
        got("S1a")
        feed(0, 2)
        both_kinds(done, "B1")
        go("S1b")
        both_kinds(done, "B2")
        go("S2b")
        got("S2a")
        got("S3a")
        feed(1536, 2)
        both_kinds(done, "B3")
        go("S3b")
        got("S0b")
        got("S1b")
        feed(3072, 1)
        got("S2b")
        got("S3b")
        feed(3840, 1)

        def finish():
            for b in range(3):
                r = pl.ds(b * 128, 128)
                outb[r, :] = (mid[r, :].astype(f32) + modrow(b, 5) * acc[r, :]).astype(bf)
            for b in range(3):
                r = pl.ds(b * 128, 128)
                load(outb.at[r, :], out_ref.at[r, :])
            for c in loads[-3:]:
                c.wait()

        finish()
        for c in copies.values():
            c.wait_send()
        all15("M").wait_send()
        all15("G").wait_send()

    any_spec = pl.BlockSpec(memory_space=pl.ANY)
    n_copies = 2 * 20 + 8 + 3 * 12 + 4 + 5 + 2
    return pl.pallas_call(
        kernel,
        out_shape=jax.ShapeDtypeStruct((384, D), bf),
        in_specs=[pl.BlockSpec(memory_space=pltpu.SMEM)] * 2 + [any_spec] * 12,
        out_specs=any_spec,
        scratch_shapes=[
            pltpu.VMEM((3, 2, 3, 4, 4, 32), f32),
            pltpu.VMEM((3, 4, 16, 64), f32),
            pltpu.VMEM((16, D), f32),
            pltpu.VMEM((256, D), f32),
            pltpu.VMEM((256, D), bf),
            pltpu.VMEM((72, D), bf),
            pltpu.VMEM((72, 1001), bf),
            pltpu.VMEM((72, 6 * D), bf),
            pltpu.VMEM((2, 3, 2, 32, 576), bf),
            pltpu.VMEM((3, 64, D), bf),
            pltpu.VMEM((3, 256, 640), f32),
            pltpu.VMEM((3, 256, 128), f32),
            pltpu.VMEM((8, 4096), f32),
            pltpu.VMEM((16, 2048), bf),
            pltpu.VMEM((16, 16, 128), bf),
            pltpu.VMEM((32, 128), bf),
            pltpu.VMEM((16, 32, 128), bf),
            pltpu.VMEM((8, 4096), f32),
            pltpu.VMEM((3, 4, 16, 64), f32),
            pltpu.VMEM((3, 4, 2, 32, D), bf),
            pltpu.VMEM((1728, D), bf),
            pltpu.VMEM((3, NKEY, D), bf),
            pltpu.VMEM((2, HID, D), bf),
            pltpu.VMEM((1280, D), bf),
            pltpu.VMEM((3, 256, 640), bf),
            pltpu.VMEM((3, 4, 2, 32, 640), bf),
            pltpu.VMEM((3, 4, 32, 640), bf),
            pltpu.VMEM((384, D), bf),
            pltpu.VMEM((384, D), bf),
            pltpu.VMEM((384, D), f32),
            pltpu.VMEM((384, D), bf),
            pltpu.SemaphoreType.DMA((n_copies,)),
            pltpu.SemaphoreType.DMA((n_copies,)),
            pltpu.SemaphoreType.DMA((18,)),
        ],
        compiler_params=pltpu.CompilerParams(
            collective_id=0, has_side_effects=True, vmem_limit_bytes=58_000_000
        ),
    )(t_index, labels, x_lo, noise, embed, tw1, tw2, table, ada, stale, wqkv, ow, fc1, fc2)


def body(
    x_lo,
    noise,
    t_index,
    labels,
    stale_kv,
    embed_w,
    t_w1,
    t_w2,
    class_table,
    ada_w,
    qkv_w,
    out_w,
    fc1_w,
    fc2_w,
):
    head_count = lax.axis_size("head")
    tile_rows, full_cols = noise.shape[1], noise.shape[2]
    batch, width = noise.shape[0], embed_w.shape[1]
    half = full_cols // head_count
    local_width = qkv_w.shape[2]
    out = fused_block(
        t_index,
        labels,
        x_lo.transpose(0, 1, 3, 2),
        noise.transpose(0, 1, 3, 2),
        embed_w,
        t_w1,
        t_w2.T,
        class_table.T,
        ada_w,
        stale_kv,
        qkv_w.transpose(1, 2, 0).reshape(3 * local_width, width),
        out_w,
        fc1_w.T,
        fc2_w.T,
    )
    return out.reshape(batch, tile_rows, half, width)


def solution(mesh):
    placed = (
        P("col", "row", "head", None),
        P("col", "row", None, None),
        P("col"),
        P("col"),
        P(None, "col", "row", None, "head"),
        P(),
        P(),
        P(None, "row"),
        P(None, "row"),
        P("row", None),
        P(None, None, "head"),
        P("head", None),
        P(None, ("col", "head")),
        P(None, ("col", "head")),
    )
    return jax.shard_map(
        body, mesh=mesh, in_specs=placed, out_specs=P("col", "row", "head", None), check_vma=False
    )
```

```python
import math

import jax
import jax.numpy as jnp
from jax import lax
from jax.experimental import pallas as pl
from jax.experimental.pallas import tpu as pltpu
from jax.sharding import PartitionSpec as P

HD = 72
TSTEPS = 1000


def fused_block(t_index, labels, x_lo, noise, embed, tw1, tw2, table, ada, stale, wqkv, ow, fc1, fc2):
    D = 1152
    L2E = 1.4426950408889634
    QS = L2E / math.sqrt(HD)
    bf, f32 = jnp.bfloat16, jnp.float32
    NKEY = 256 + 15 * 64
    HID = 4608
    UNROLL = 4
    EARLY = 256 + 9 * 64

    def kernel(
        t_s, label_s, x_h, noise_h, embed_h, tw1_h, tw2_h, table_h, ada_h, stale_h, wqkv_h, ow_h, fc1_h,
        fc2_h, out_ref, xn, nz, emb, pos, tw1, tw2, table, ada, skv, kown, att1, mass1, part, pieces, rsb, both_ref, gs, modp, noisy,
        tok, wq, kvb, wb, owb, qb, att, attr, n2, mid, acc, outb, send, recv, local,
    ):
        row, col, head = lax.axis_index("row"), lax.axis_index("col"), lax.axis_index("head")
        z, core = row // 2, row % 2
        x, y = head * 2 + col // 4, col % 4

        def at(x_, y_, z_, core_):
            return (z_ * 2 + core_, (x_ % 2) * 4 + y_, x_ // 2)

        peers = {
            "sib": at(x, y, z, 1 - core),
            "zp": at(x, y, (z + 1) % 8, core),
            "zm": at(x, y, (z + 7) % 8, core),
            "ap": at((x + core) % 4, (y + 1 - core) % 4, z, core),
            "am": at((x + 4 - core) % 4, (y + 3 + core) % 4, z, core),
            "bp": at((x + 1 - core) % 4, (y + core) % 4, z, core),
            "bm": at((x + 3 + core) % 4, (y + 4 - core) % 4, z, core),
            "far": at((x + 2) % 4, y, z, core),
        }
        other = at(3 - x, y, z, core)
        twin = at(x, y, z + 1 - 2 * (z % 2), core)
        near = {}
        for dr in (1, 15):
            near[f"h{dr}"] = ((row + dr) % 16, col, 1 - head)
        fellows = {k: ((row + k) % 16, col, head) for k in range(1, 16)}

        copies = {}
        order = {"n": 0}

        def remote(name, src, dst, peer):
            k = order["n"]
            order["n"] = k + 1
            c = pltpu.make_async_remote_copy(
                src_ref=src, dst_ref=dst, send_sem=send.at[k], recv_sem=recv.at[k],
                device_id=peer, device_id_type=pl.DeviceIdType.MESH,
            )
            copies[name] = c
            return c

        def go(name):
            copies[name].start()

        def got(name):
            copies[name].wait_recv()

        loads = []

        def load(src, dst):
            c = pltpu.make_async_copy(src, dst, local.at[len(loads)])
            loads.append(c)
            c.start()
            return c

        SIZE, PLUS = {"": 112, "E": 32}, {"": 64, "E": 16}

        def blk(kind, group, j, part=None):
            lo, n = {
                None: (0, SIZE[kind]), 0: (0, PLUS[kind]), 1: (PLUS[kind], SIZE[kind] - PLUS[kind])
            }[part]
            if j < 3:
                base = group * 864 + (336 if kind else 0) + j * SIZE[kind]
            else:
                base = 3456 + group * 288 + (112 if kind else 0)
            return wb.at[:, pl.ds(base + lo, n), :]

        def ring(tag, sides, place):
            p, m = sides
            remote(tag + "1", place(0, None), place(1, None), p)
            remote(tag + "2", place(0, None), place(2, None), m)
            remote(tag + "3a", place(1, 0), place(3, 0), p)
            remote(tag + "3b", place(2, 1), place(3, 1), m)

        along = {
            "A": (peers["ap"], peers["am"]),
            "B": (peers["bp"], peers["bm"]),
            "EA": (at((x + 1) % 4, y, z, core), at((x + 3) % 4, y, z, core)),
            "EB": (at(x, (y + 1) % 4, z, core), at(x, (y + 3) % 4, z, core)),
        }
        for kind in ("", "E"):
            ring(kind + "A", along[kind + "A"], lambda g, part, kind=kind: blk(kind, g, 0, part))
            for g in range(4):
                ring(
                    f"{kind}B{g}", along[kind + "B"],
                    lambda j, part, g=g, kind=kind: blk(kind, g, j, part),
                )
        for g in range(4):
            for name, lo, n in ((f"S{g}a", g * 864, 432), (f"S{g}b", 3456 + g * 288, 144)):
                remote(
                    name, wb.at[:, pl.ds(lo, n), :], wb.at[:, pl.ds(lo + n, n), :], peers["sib"]
                )

        def slot(b, s, lo=0, n=64):
            return kvb.at[b, pl.ds(256 + s * 64 + lo, n), :]

        for b in range(3):
            own = kown.at[b]
            zp, zm = peers["zp"], peers["zm"]
            right, left = (0, 2, 9), (1, 3, 10)
            remote(f"R1_{b}", own, slot(b, 0), zp)
            remote(f"L1_{b}", own, slot(b, 1), zm)
            for d in (1, 2):
                remote(f"R{d + 1}_{b}", slot(b, right[d - 1]), slot(b, right[d]), zp)
                remote(f"L{d + 1}_{b}", slot(b, left[d - 1]), slot(b, left[d]), zm)
            remote(f"R4_{b}", slot(b, 9, 0, 32), slot(b, 11, 0, 32), zp)
            remote(f"L4_{b}", slot(b, 10, 32, 32), slot(b, 11, 32, 32), zm)
            remote(f"C0_{b}", own, slot(b, 4), peers["sib"])
            remote(f"C1_{b}", slot(b, 0, 0, 256), slot(b, 5, 0, 256), peers["sib"])
            remote(f"C2_{b}", slot(b, 9, 0, 192), slot(b, 12, 0, 192), peers["sib"])
            remote(
                f"X{b}", att.at[b, :, 1 - head], attr.at[b], peers["far"],
            )
        part_at = lambda p: p * 288 + core * 144
        ow_own = pl.ds(pl.multiple_of(part_at(z % 2), 16), 144)
        far0 = pl.ds(pl.multiple_of(704 + part_at(z % 2), 16), 144)
        far1 = pl.ds(pl.multiple_of(704 + part_at(1 - z % 2), 16), 144)
        remote("O", ow_h.at[ow_own, :], owb.at[far0, :], other)
        remote("OZ", owb.at[far0, :], owb.at[far0, :], twin)
        remote("OS0", owb.at[far0, :], owb.at[far0, :], peers["sib"])
        remote("OS1", owb.at[far1, :], owb.at[far1, :], peers["sib"])
        remote("Pf", xn.at[1, head], xn.at[1, head], peers["far"])
        remote("Pd", xn.at[1, head], xn.at[0, head], fellows[1])
        remote("Pu", xn.at[1, head], xn.at[2, head], fellows[15])
        remote("Pdf", xn.at[1, head], xn.at[0, head], near["h1"])
        remote("Puf", xn.at[1, head], xn.at[2, head], near["h15"])
        shared = {}
        for tag in "MG":
            shared[tag] = order["n"]
            order["n"] += 1
        to_all = {"M": [], "G": []}
        for k in range(1, 16):
            to = (row + k) % 16
            chunk = pl.ds(pl.multiple_of(to * 128, 128), 128)
            for tag, src, dst in (
                ("M", pieces.at[:, chunk], rsb.at[k]), ("G", both_ref, gs.at[k])
            ):
                to_all[tag].append(
                    pltpu.make_async_remote_copy(
                        src_ref=src, dst_ref=dst, send_sem=send.at[shared[tag]],
                        recv_sem=recv.at[shared[tag]], device_id=fellows[k],
                        device_id_type=pl.DeviceIdType.MESH,
                    )
                )

        def all15(tag):
            buf = {"M": rsb, "G": gs}[tag].at[pl.ds(1, 15)]
            return pltpu.make_async_remote_copy(
                src_ref=buf, dst_ref=buf, send_sem=send.at[shared[tag]],
                recv_sem=recv.at[shared[tag]], device_id=fellows[1],
                device_id_type=pl.DeviceIdType.MESH,
            )

        c_w = []
        for kind, lo in (("", 0), ("E", 112)):
            rows = pl.ds(pl.multiple_of(core * 144 + lo, 16), SIZE[kind])
            for k, w_h in enumerate((fc1_h, fc2_h)):
                c_w.append(load(w_h.at[rows, :], wb.at[k, pl.ds(336 if kind else 0, SIZE[kind]), :]))
        c_x = load(x_h, xn.at[1, head])
        c_tw1 = load(tw1_h, tw1)
        c_tw2 = load(tw2_h, tw2)
        c_table = load(table_h, table)
        c_ada = load(ada_h, ada)
        c_skv = load(stale_h, skv)
        c_nz = load(noise_h, nz)
        c_emb = load(embed_h, emb)
        c_wq = load(wqkv_h, wq)
        c_ow = load(ow_h, owb.at[pl.ds(64, 576), :])
        barrier = pltpu.get_barrier_semaphore()
        greet = list(fellows.values()) + list(near.values())
        greet += [peers[n] for n in ("ap", "am", "bp", "bm", "far")]
        for peer in greet:
            pl.semaphore_signal(barrier, inc=1, device_id=peer, device_id_type=pl.DeviceIdType.MESH)
        owb[pl.ds(0, 64), :] = jnp.zeros((64, D), bf)
        owb[pl.ds(640, 64), :] = jnp.zeros((64, D), bf)
        att[...] = jnp.zeros_like(att)
        att1[...] = jnp.zeros_like(att1)
        mass1[...] = jnp.zeros_like(mass1)
        c_skv.wait()
        for b in range(3):
            kown[b] = jnp.concatenate([skv[0, b], skv[1, b]], axis=-1).reshape(64, D)
        def by_image(values, shape):
            r = lax.broadcasted_iota(jnp.int32, shape, 0)
            return jnp.where(r == 0, values[0], jnp.where(r == 1, values[1], values[2]))

        ts = [t_s[b] for b in range(3)]
        k128 = lax.broadcasted_iota(jnp.int32, (8, 128), 1).astype(f32)
        angles = by_image(ts, (8, 128)).astype(f32) * jnp.exp(-math.log(10000.0) * k128 / 128)
        feats = jnp.concatenate([jnp.cos(angles), jnp.sin(angles)], axis=1).astype(bf)
        c_tw1.wait()
        hid = jnp.dot(feats, tw1[...], preferred_element_type=f32)
        hid = (hid * jax.nn.sigmoid(hid)).astype(bf)
        c_tw2.wait()
        c_table.wait()
        NT = (((1,), (1,)), ((), ()))
        kinds = lax.broadcasted_iota(jnp.int32, (8, 1001), 1)
        picked = kinds == by_image([label_s[b] for b in range(3)], (8, 1001))
        cond = lax.dot_general(hid, tw2[...], NT, preferred_element_type=f32)
        cond = cond + lax.dot_general(
            picked.astype(f32).astype(bf), table[...], NT, preferred_element_type=f32
        )
        cond = (cond * jax.nn.sigmoid(cond)).astype(bf)
        c_ada.wait()
        for k in range(2):
            first = jnp.dot(cond, ada[:, pl.ds(k * 3 * D, 3 * D)], preferred_element_type=f32)
            part[pl.ds(4 * k, 4), pl.ds(0, 3 * D)] = first[0:4]
        for r in range(16):
            pieces[:, pl.ds(r * 128, 128)] = jnp.concatenate(
                [part[:, pl.ds(r * 256, 128)], part[:, pl.ds(r * 256 + 128, 128)]], axis=0
            ).astype(bf)
        steps = lax.broadcasted_iota(jnp.int32, (8, TSTEPS), 1)
        betas = 0.0001 + (0.02 - 0.0001) * steps.astype(f32) / (TSTEPS - 1)
        logs = jnp.where(steps <= by_image(ts, (8, TSTEPS)), jnp.log(1.0 - betas), 0.0)
        abar = jnp.exp(jnp.sum(logs, axis=1, keepdims=True))

        def wide(column):
            return jnp.stack([jnp.broadcast_to(column[b : b + 1], (4, 64)) for b in range(3)])

        keep, fuzz = wide(jnp.sqrt(abar)), wide(jnp.sqrt(1.0 - abar))

        def waves(n, start):
            place = (lax.broadcasted_iota(jnp.int32, (n, D // 4), 0) + start).astype(f32)
            k = lax.broadcasted_iota(jnp.int32, (n, D // 4), 1).astype(f32)
            args = place * jnp.exp(-math.log(10000.0) * k / (D // 4))
            return jnp.concatenate([jnp.sin(args), jnp.cos(args)], axis=1)

        rp, cp = waves(8, row * 4), waves(64, 0)
        for i in range(4):
            pos[pl.ds(i * 64, 64), :] = jnp.concatenate(
                [jnp.broadcast_to(rp[i : i + 1], (64, D // 2)), cp], axis=1
            )
        c_x.wait()
        pl.semaphore_wait(barrier, len(greet))
        for n in ("Pf", "Pd", "Pu", "Pdf", "Puf"):
            go(n)
        for c in to_all["M"]:
            c.start()
        go("R1_0")
        go("L1_0")
        for c in c_w:
            c.wait()
        for n in ("A1", "A2", "EA1", "EA2", "O", "B01", "B02", "EB01", "EB02"):
            go(n)
        for b in range(3):
            go(f"C0_{b}")
        c_nz.wait()
        c_emb.wait()
        for n in ("Pf", "Pd", "Pu", "Pdf", "Puf"):
            got(n)

        def line(d, i):
            return jnp.concatenate([xn[d, 0, :, i], xn[d, 1, :, i]], axis=-1)

        lines = [line(0, 3)] + [line(1, i) for i in range(4)] + [line(2, 0)]
        lines[0] = jnp.where(row == 0, lines[1], lines[0])
        lines[5] = jnp.where(row == 15, lines[4], lines[5])
        total = jnp.zeros((3, 4, 64), f32)
        square = jnp.zeros((3, 4, 64), f32)
        for i in range(4):
            for di in range(2):
                v = 0.75 * lines[i + 1] + 0.25 * lines[i + 2 * di]
                sides = (
                    jnp.concatenate([v[:, :, :1], v[:, :, :63]], axis=-1),
                    jnp.concatenate([v[:, :, 1:], v[:, :, 63:]], axis=-1),
                )
                for dj in range(2):
                    k = 2 * di + dj
                    n = keep * (0.75 * v + 0.25 * sides[dj]) + fuzz * nz[:, i, 4 * k : 4 * k + 4, :]
                    noisy[:, i, 4 * k : 4 * k + 4, :] = n
                    total = total + n
                    square = square + n * n
        lane1 = lax.broadcasted_iota(jnp.int32, (8, 128), 1)
        head_mid = jnp.zeros((8, 128), f32), jnp.zeros((8, 128), f32)
        for b in range(3):
            s = jnp.concatenate(
                [
                    jnp.sum(total[b], axis=1, keepdims=True),
                    jnp.sum(square[b], axis=1, keepdims=True),
                ],
                axis=0,
            )
            s = jnp.broadcast_to(s, (8, 128))
            s1 = s.astype(bf).astype(f32)
            s2 = (s - s1).astype(bf).astype(f32)
            s3 = s - s1 - s2
            head_mid = (
                jnp.where(lane1 == b, s1, jnp.where(lane1 == b + 3, s3, head_mid[0])),
                jnp.where(lane1 == b, s2, head_mid[1]),
            )
        sums = jnp.concatenate(head_mid, axis=0).astype(bf)
        both_ref[pl.ds(16, 16), :] = sums
        all15("M").wait_recv()
        at0 = pl.multiple_of(row * 256, 128)
        piece = jnp.concatenate(
            [part[:, pl.ds(at0, 128)], part[:, pl.ds(pl.multiple_of(at0 + 128, 128), 128)]], axis=0
        )
        for k in range(1, 16):
            piece = piece + rsb[k].astype(f32)
        piece = piece.astype(bf)
        both_ref[pl.ds(0, 16), :] = piece
        gs[0] = jnp.concatenate([piece, sums], axis=0)
        for c in to_all["G"]:
            c.start()
        for b in (1, 2):
            go(f"R1_{b}")
            go(f"L1_{b}")

        def norm(v):
            centre = jnp.mean(v, axis=-1, keepdims=True)
            v = v - centre
            spread = jnp.mean(v * v, axis=-1, keepdims=True)
            return v * lax.rsqrt(spread + 1e-06)

        def modrow(b, k):
            return modp[pl.ds(b + 4 * (k // 3), 1), pl.ds((k % 3) * D, D)]

        def qkv(b):
            n1 = (
                norm(tok[b].reshape(256, D).astype(f32)) * (1.0 + modrow(b, 1)) + modrow(b, 0)
            ).astype(bf)
            q = lax.dot_general(n1, wq[pl.ds(0, 576), :], NT, preferred_element_type=f32)
            qb[b, :, pl.ds(0, 576)] = (q * QS).astype(bf)
            kv = lax.dot_general(n1, wq[pl.ds(576, 1152), :], NT, preferred_element_type=f32)
            kvb[b, pl.ds(0, 256), :] = kv.astype(bf)

        lane = lax.broadcasted_iota(jnp.int32, (1, 256), 1)

        lane128 = lax.broadcasted_iota(jnp.int32, (1, 128), 1)

        def attend(b, late):
            keys = pl.ds(EARLY, NKEY - EARLY) if late else pl.ds(0, EARLY)

            def score(h):
                first = h * HD
                ks = pl.multiple_of((first // 128) * 128, 128)
                off = first - ks
                here = (lane >= off) & (lane < off + HD)
                q = qb[b, :, pl.ds(ks, 256)]
                q = jnp.where(here, q, jnp.zeros_like(q))
                return lax.dot_general(
                    q, kvb[b, keys, pl.ds(ks, 256)], NT, preferred_element_type=f32
                )

            def mix(h, s):
                first = h * HD
                vs = pl.multiple_of(jnp.minimum(((576 + first) // 128) * 128, 896), 128)
                voff = 576 + first - vs
                mine = (lane >= voff) & (lane < voff + HD)
                cols = pl.ds(pl.multiple_of(vs - 512, 128), 256)
                chosen = lane128 == h
                if late:
                    top = jnp.max(s, axis=1, keepdims=True) + 2.0
                    before = jnp.sum(jnp.where(chosen, mass1[b], 0.0), axis=1, keepdims=True)
                    top = jnp.maximum(top, before)
                    p = jnp.exp2(s - (top - 2.0))
                    kept = jnp.exp2(before - top)
                    mass = jnp.sum(p, axis=1, keepdims=True) + kept
                    o = jnp.dot(p.astype(bf), kvb[b, keys, pl.ds(vs, 256)], preferred_element_type=f32)
                    o = (o + kept * att1[b, :, cols]) * (1.0 / mass)
                    o = o.astype(bf).reshape(4, 2, 32, 256)
                    att[b, :, :, :, cols] = jnp.where(
                        mine.reshape(1, 1, 1, 256), o, att[b, :, :, :, cols]
                    )
                    return
                fresh, old = s[:, :256], s[:, 256:]
                top = jnp.maximum(
                    jnp.max(fresh, axis=1, keepdims=True), jnp.max(old, axis=1, keepdims=True) + 2.0
                )
                p0 = jnp.exp2(fresh - top)
                p1 = jnp.exp2(old - (top - 2.0))
                mass = jnp.sum(p0, axis=1, keepdims=True) + jnp.sum(p1, axis=1, keepdims=True)
                o = jnp.dot(
                    p0.astype(bf), kvb[b, pl.ds(0, 256), pl.ds(vs, 256)],
                    preferred_element_type=f32,
                ) + jnp.dot(
                    p1.astype(bf), kvb[b, pl.ds(256, EARLY - 256), pl.ds(vs, 256)],
                    preferred_element_type=f32,
                )
                att1[b, :, cols] = jnp.where(mine, o * (1.0 / mass), att1[b, :, cols])
                mass1[b] = jnp.where(chosen, top + jnp.log2(mass), mass1[b])

            def some(i, _):
                hs = [i * UNROLL + j for j in range(UNROLL)]
                ss = [score(h) for h in hs]
                for h, s in zip(hs, ss):
                    mix(h, s)
                return 0

            lax.fori_loop(0, 8 // UNROLL, some, 0)

        def project(b):
            rows = pl.ds(b * 128, 128)
            p = acc[rows, :] + jnp.dot(attr[b].reshape(128, 640), owb[pl.ds(640, 640), :], preferred_element_type=f32)
            t = tok[b, :, head].reshape(128, D).astype(f32)
            m = (t + modrow(b, 2) * p).astype(bf)
            mid[pl.ds(b * 128, 128), :] = m
            n = norm(m.astype(f32)) * (1.0 + modrow(b, 4)) + modrow(b, 3)
            n2[pl.ds(b * 128, 128), :] = n.astype(bf)
            acc[rows, :] = jnp.zeros((128, D), f32)

        def project_own(b):
            mine = att[b, :, head].reshape(128, 640)
            acc[pl.ds(b * 128, 128), :] = jnp.dot(
                mine, owb[pl.ds(0, 640), :], preferred_element_type=f32
            )

        def feed(first, count):
            rows = [pl.ds(first + i * 768, 768) for i in range(count)]
            hids = [
                lax.dot_general(n2[...], wb[0, r, :], NT, preferred_element_type=f32) for r in rows
            ]
            for r, hid in zip(rows, hids):
                hid = jax.nn.gelu(hid, approximate=True).astype(bf)
                acc[...] += jnp.dot(hid, wb[1, r, :], preferred_element_type=f32)

        def kstep(d, b):
            got(f"R{d}_{b}")
            got(f"L{d}_{b}")
            if d < 4:
                go(f"R{d + 1}_{b}")
                go(f"L{d + 1}_{b}")

        def fwd(tag):
            got(tag + "1")
            go(tag + "3a")
            got(tag + "2")
            go(tag + "3b")

        def done(tag):
            got(tag + "3a")
            got(tag + "3b")

        kstep(1, 0)
        all15("G").wait_recv()
        first, second = jnp.zeros((8, 128), f32), jnp.zeros((8, 128), f32)
        for k in range(16):
            g = gs[k].astype(f32)
            first, second = first + g[16:24], second + g[24:32]
            lo = pl.multiple_of(((row + 16 - k) % 16) * 256, 128)
            modp[:, pl.ds(lo, 128)] = g[0:8]
            modp[:, pl.ds(pl.multiple_of(lo + 128, 128), 128)] = g[8:16]
        shares, gains = [], []
        for b in range(3):
            chosen = jnp.where((lane1 == b) | (lane1 == b + 3), first, 0.0)
            chosen = chosen + jnp.where(lane1 == b, second, 0.0)
            col_b = jnp.sum(chosen, axis=1, keepdims=True) / 16384.0
            centre = col_b[0:4]
            gain = lax.rsqrt(col_b[4:8] - centre * centre + 1e-05)
            shares.append(jnp.concatenate([centre] * 4, axis=0))
            gains.append(jnp.concatenate([gain] * 4, axis=0))
        whi = emb[...].astype(bf)
        wlo = (emb[...] - whi.astype(f32)).astype(bf)
        w3 = jnp.concatenate([whi, whi, wlo], axis=0)
        c_wq.wait()
        for b in range(3):
            for i in range(4):
                n = (noisy[b, i] - shares[b]) * gains[b]
                hi = n.astype(bf)
                lo = (n - hi.astype(f32)).astype(bf)
                e = lax.dot_general(
                    jnp.concatenate([hi, lo, hi], axis=0), w3, (((0,), (0,)), ((), ())),
                    preferred_element_type=f32,
                )
                e = (e + pos[pl.ds(i * 64, 64), :]).astype(bf)
                tok[b, i] = e.reshape(2, 32, D)
        def both_kinds(act, tag):
            act(tag)
            act("E" + tag)

        def begin(tag):
            go(tag + "1")
            go(tag + "2")

        kstep(1, 1)
        qkv(0)
        kstep(1, 2)
        both_kinds(fwd, "A")
        for g in (1, 2):
            both_kinds(begin, f"B{g}")
        qkv(1)
        kstep(2, 0)
        go("C1_0")
        qkv(2)
        kstep(2, 1)
        go("C1_1")
        got("C0_0")
        got("C1_0")
        attend(0, False)
        kstep(2, 2)
        go("C1_2")
        both_kinds(fwd, "B0")
        both_kinds(done, "A")
        both_kinds(begin, "B3")
        got("C0_1")
        got("C1_1")
        kstep(3, 0)
        attend(1, False)
        kstep(3, 1)
        go("S0a")
        got("C0_2")
        got("C1_2")
        attend(2, False)
        kstep(3, 2)
        kstep(4, 0)
        go("C2_0")
        kstep(4, 1)
        go("C2_1")
        got("O")
        go("OZ")
        go("OS0")
        got("C2_0")
        attend(0, True)
        go("X0")
        kstep(4, 2)
        go("C2_2")
        both_kinds(fwd, "B1")
        got("C2_1")
        attend(1, True)
        go("X1")
        both_kinds(done, "B0")
        go("S0b")
        go("S1a")
        got("C2_2")
        attend(2, True)
        go("X2")
        both_kinds(fwd, "B2")
        go("S2a")
        c_ow.wait()
        project_own(0)
        project_own(1)
        got("OZ")
        go("OS1")
        project_own(2)
        got("OS0")
        got("X0")
        got("OS1")
        project(0)
        got("X1")
        project(1)
        both_kinds(fwd, "B3")
        go("S3a")
        got("X2")
        project(2)
        got("S0a")
        got("S1a")
        feed(0, 2)
        both_kinds(done, "B1")
        go("S1b")
        both_kinds(done, "B2")
        go("S2b")
        got("S2a")
        got("S3a")
        feed(1536, 2)
        both_kinds(done, "B3")
        go("S3b")
        got("S0b")
        got("S1b")
        feed(3072, 1)
        got("S2b")
        got("S3b")
        feed(3840, 1)

        def finish():
            for b in range(3):
                r = pl.ds(b * 128, 128)
                outb[r, :] = (mid[r, :].astype(f32) + modrow(b, 5) * acc[r, :]).astype(bf)
            for b in range(3):
                r = pl.ds(b * 128, 128)
                load(outb.at[r, :], out_ref.at[r, :])
            for c in loads[-3:]:
                c.wait()

        finish()
        for c in copies.values():
            c.wait_send()
        all15("M").wait_send()
        all15("G").wait_send()

    any_spec = pl.BlockSpec(memory_space=pl.ANY)
    n_copies = 2 * 20 + 8 + 3 * 12 + 4 + 5 + 2
    return pl.pallas_call(
        kernel,
        out_shape=jax.ShapeDtypeStruct((384, D), bf),
        in_specs=[pl.BlockSpec(memory_space=pltpu.SMEM)] * 2 + [any_spec] * 12,
        out_specs=any_spec,
        scratch_shapes=[
            pltpu.VMEM((3, 2, 3, 4, 4, 32), f32),
            pltpu.VMEM((3, 4, 16, 64), f32),
            pltpu.VMEM((16, D), f32),
            pltpu.VMEM((256, D), f32),
            pltpu.VMEM((256, D), bf),
            pltpu.VMEM((72, D), bf),
            pltpu.VMEM((72, 1001), bf),
            pltpu.VMEM((72, 6 * D), bf),
            pltpu.VMEM((2, 3, 2, 32, 576), bf),
            pltpu.VMEM((3, 64, D), bf),
            pltpu.VMEM((3, 256, 640), f32),
            pltpu.VMEM((3, 256, 128), f32),
            pltpu.VMEM((8, 4096), f32),
            pltpu.VMEM((16, 2048), bf),
            pltpu.VMEM((16, 16, 128), bf),
            pltpu.VMEM((32, 128), bf),
            pltpu.VMEM((16, 32, 128), bf),
            pltpu.VMEM((8, 4096), f32),
            pltpu.VMEM((3, 4, 16, 64), f32),
            pltpu.VMEM((3, 4, 2, 32, D), bf),
            pltpu.VMEM((1728, D), bf),
            pltpu.VMEM((3, NKEY, D), bf),
            pltpu.VMEM((2, HID, D), bf),
            pltpu.VMEM((1280, D), bf),
            pltpu.VMEM((3, 256, 640), bf),
            pltpu.VMEM((3, 4, 2, 32, 640), bf),
            pltpu.VMEM((3, 4, 32, 640), bf),
            pltpu.VMEM((384, D), bf),
            pltpu.VMEM((384, D), bf),
            pltpu.VMEM((384, D), f32),
            pltpu.VMEM((384, D), bf),
            pltpu.SemaphoreType.DMA((n_copies,)),
            pltpu.SemaphoreType.DMA((n_copies,)),
            pltpu.SemaphoreType.DMA((18,)),
        ],
        compiler_params=pltpu.CompilerParams(
            collective_id=0, has_side_effects=True, vmem_limit_bytes=58_000_000
        ),
    )(t_index, labels, x_lo, noise, embed, tw1, tw2, table, ada, stale, wqkv, ow, fc1, fc2)


def body(
    x_lo,
    noise,
    t_index,
    labels,
    stale_kv,
    embed_w,
    t_w1,
    t_w2,
    class_table,
    ada_w,
    qkv_w,
    out_w,
    fc1_w,
    fc2_w,
):
    head_count = lax.axis_size("head")
    tile_rows, full_cols = noise.shape[1], noise.shape[2]
    batch, width = noise.shape[0], embed_w.shape[1]
    half = full_cols // head_count
    local_width = qkv_w.shape[2]
    out = fused_block(
        t_index,
        labels,
        x_lo.transpose(0, 1, 3, 2),
        noise.transpose(0, 1, 3, 2),
        embed_w,
        t_w1,
        t_w2.T,
        class_table.T,
        ada_w,
        stale_kv,
        qkv_w.transpose(1, 2, 0).reshape(3 * local_width, width),
        out_w,
        fc1_w.T,
        fc2_w.T,
    )
    return out.reshape(batch, tile_rows, half, width)


def solution(mesh):
    placed = (
        P("col", "row", "head", None),
        P("col", "row", None, None),
        P("col"),
        P("col"),
        P(None, "col", "row", None, "head"),
        P(),
        P(),
        P(None, "row"),
        P(None, "row"),
        P("row", None),
        P(None, None, "head"),
        P("head", None),
        P(None, ("col", "head")),
        P(None, ("col", "head")),
    )
    return jax.shard_map(
        body, mesh=mesh, in_specs=placed, out_specs=P("col", "row", "head", None), check_vma=False
    )
```
